256 devices in a mesh: gx: 4 (over x_hi, core), gy: 8 (over y, x_lo), gz: 8 (over z).
Axes of the slice: x: 4 (x_hi: 2, x_lo: 2; x = x_hi * 2 + x_lo), y: 4, z: 8, core: 2. Of those that a mesh axis runs over, the one named last changes fastest.
Arguments:
- node_feats: bfloat16 [64, 128, 256, 128], P('gx', 'gy', 'gz'), may hold values from -6 to 6
- node_type: int32 [64, 128, 256], P('gx', 'gy', 'gz'), may hold values from 0 to 3
- boundary_code: int32 [64, 128, 256], P('gx', 'gy', 'gz'), may hold values from 0 to 2
- wall_flag: int32 [64, 128, 256], P('gx', 'gy', 'gz'), may hold values from 0 to 1, as said below
- type_table: float32 [4, 128], replicated, may hold values from -3 to 3
- boundary_table: float32 [3, 128], replicated, may hold values from -3 to 3
- edge_self: bfloat16 [2, 128, 128], replicated, may hold values from -0.5 to 0.5
- edge_neighbour: bfloat16 [2, 128, 128], replicated, may hold values from -0.5 to 0.5
- edge_bias: float32 [2, 6, 128], replicated, may hold values from -3 to 3
- edge_out: bfloat16 [2, 128, 128], replicated, may hold values from -0.5 to 0.5
- node_self: bfloat16 [2, 128, 128], replicated, may hold values from -0.5 to 0.5
- node_aggregate: bfloat16 [2, 128, 128], replicated, may hold values from -0.5 to 0.5
- node_out: bfloat16 [2, 128, 128], replicated, may hold values from -0.5 to 0.5
- node_gain: float32 [2, 128], replicated, may hold values from 0.25 to 1.75
Outputs:
- latent: bfloat16 [64, 128, 256, 128], P('gx', 'gy', 'gz')
- wall_mean: float32 [128], replicated
The draws below stay inside these ranges and needn't reach their ends.
Inputs may be any that keep to these rules, and one draw needn't show every extreme that they name: Every node whose wall-normal index is 0 or 127 has wall_flag 1.
All inputs are finite; a program needn't handle non-finite values.
Results may differ from the reference program's by a relative error of at most 0.012.
Values may be sent and summed in bfloat16 or wider, within the bound.
A program may use at most 128 MiB of HBM per device.

```python
import jax
import jax.numpy as jnp
from jax import lax

H = 128
LAYERS = 2
NTYPES = 4
NCODES = 3
NX = 64
NY = 128
NZ = 256


def draw_wall_flag(key, part):
    picks = jax.random.randint(jax.random.fold_in(key, 17), (NX, NY, NZ), 0, 8)
    rows_y = jnp.arange(NY, dtype=jnp.int32)[None, :, None]
    on_wall = jnp.logical_or(rows_y == 0, rows_y == NY - 1)
    flagged = jnp.logical_or(picks == 0, on_wall)
    return flagged.astype(jnp.int32)


def plant(array, own_key, least, largest):
    shape = array.shape
    spot = [jax.random.randint(jax.random.fold_in(own_key, axis), (), 0, shape[axis]) for axis in range(len(shape))]
    array = array.at[tuple(spot)].set(least)
    longest = shape.index(max(shape))
    spot[longest] = (spot[longest] + 1) % shape[longest]
    return array.at[tuple(spot)].set(largest)


def block_levels(key, extent, cuts, smallest, high):
    def one(dim, parts):
        draws = jax.random.uniform(jax.random.fold_in(jax.random.fold_in(key, 6), dim), (parts,), jnp.float32, smallest / len(cuts), high / len(cuts))
        return jnp.repeat(jnp.exp(draws), extent[dim] // parts).reshape((-1,) + (1,) * (len(extent) - dim - 1))

    gain = one(*cuts[0])
    for cut in cuts[1:]:
        gain = gain * one(*cut)
    return gain


def scatter_about(key, shape, scale, reach, pieces=(), held_as=jnp.bfloat16):
    level = block_levels(key, shape, pieces, -0.22, 0.18) if pieces else 1.0
    entries = jax.random.normal(key, shape, jnp.float32) * scale * level
    return jnp.minimum(jnp.maximum(entries, -reach), reach).astype(held_as)


def setup_inputs(seed: int = 0) -> dict:
    splits = jax.random.split(jax.random.key(seed), 15)
    return {
        "node_feats": scatter_about(splits[0], (NX, NY, NZ, H), 1.0, 6.0, ((0, 4), (1, 8), (2, 8))),
        "node_type": plant(jax.random.randint(splits[1], (NX, NY, NZ), 0, NTYPES), jax.random.fold_in(splits[1], 1), 0, NTYPES - 1).astype(jnp.int32),
        "boundary_code": plant(jax.random.randint(splits[2], (NX, NY, NZ), 0, NCODES), jax.random.fold_in(splits[2], 1), 0, NCODES - 1).astype(jnp.int32),
        "wall_flag": draw_wall_flag(jax.random.fold_in(splits[14], 71), 0),
        "type_table": scatter_about(splits[4], (NTYPES, H), 0.5, 3.0, (), jnp.float32),
        "boundary_table": scatter_about(splits[5], (NCODES, H), 0.5, 3.0, (), jnp.float32),
        "edge_self": scatter_about(splits[6], (LAYERS, H, H), H ** -0.5, 0.5),
        "edge_neighbour": scatter_about(splits[7], (LAYERS, H, H), H ** -0.5, 0.5),
        "edge_bias": scatter_about(splits[8], (LAYERS, 6, H), 0.5, 3.0, (), jnp.float32),
        "edge_out": scatter_about(splits[9], (LAYERS, H, H), H ** -0.5, 0.5),
        "node_self": scatter_about(splits[10], (LAYERS, H, H), H ** -0.5, 0.5),
        "node_aggregate": scatter_about(splits[11], (LAYERS, H, H), H ** -0.5, 0.5),
        "node_out": scatter_about(splits[12], (LAYERS, H, H), H ** -0.5, 0.5),
        "node_gain": jnp.clip(1.0 + 0.15 * jax.random.normal(splits[13], (LAYERS, H), jnp.float32), 0.25, 1.75),
    }


epsilon = 1e-05

def reference(node_feats, node_type, boundary_code, wall_flag, type_table, boundary_table, edge_self, edge_neighbour, edge_bias, edge_out, node_self, node_aggregate, node_out, node_gain):
    latent = (node_feats.astype(jnp.float32) + type_table[node_type] + boundary_table[boundary_code]).astype(jnp.bfloat16)
    rows_y = jnp.arange(NY)
    lower_ok = (rows_y >= 1).astype(jnp.float32)[None, :, None, None]
    upper_ok = (rows_y < NY - 1).astype(jnp.float32)[None, :, None, None]
    for which_layer in range(LAYERS):
        selfpart = jnp.dot(latent, edge_self[which_layer], preferred_element_type=jnp.float32)
        sendpart = jnp.dot(latent, edge_neighbour[which_layer], preferred_element_type=jnp.float32).astype(jnp.bfloat16)
        shifts = [(1, 0), (-1, 0), (1, 1), (-1, 1), (1, 2), (-1, 2)]
        masks = [None, None, lower_ok, upper_ok, None, None]
        aggregate = jnp.zeros(selfpart.shape, jnp.float32)
        for direction in range(6):
            neighbour = jnp.roll(sendpart, shifts[direction][0], axis=shifts[direction][1])
            hidden = jax.nn.silu(selfpart + neighbour.astype(jnp.float32) + edge_bias[which_layer, direction]).astype(jnp.bfloat16)
            message = jnp.dot(hidden, edge_out[which_layer], preferred_element_type=jnp.float32)
            if masks[direction] is not None:
                message = message * masks[direction]
            aggregate = aggregate + message
        aggregate = aggregate.astype(jnp.bfloat16)
        before = jnp.dot(latent, node_self[which_layer], preferred_element_type=jnp.float32) + jnp.dot(aggregate, node_aggregate[which_layer], preferred_element_type=jnp.float32)
        inner = jax.nn.silu(before).astype(jnp.bfloat16)
        update = jnp.dot(inner, node_out[which_layer], preferred_element_type=jnp.float32)
        centre = lax.optimization_barrier(jnp.mean(update, axis=-1, keepdims=True))
        spread = lax.optimization_barrier(jnp.mean(jnp.square(update - centre), axis=-1, keepdims=True))
        normed = (update - centre) * jax.lax.rsqrt(spread + epsilon) * node_gain[which_layer]
        latent = (latent.astype(jnp.float32) + normed).astype(jnp.bfloat16)
    flags = wall_flag.astype(jnp.float32)
    wall_sum = lax.optimization_barrier(jnp.sum(latent.astype(jnp.float32) * flags[..., None], axis=(0, 1, 2)))
    wall_count = jnp.sum(flags)
    return (latent, wall_sum / wall_count)
```

```python
import functools

import jax
import jax.numpy as jnp
from jax import lax
from jax.experimental import pallas as pl
from jax.experimental.pallas import tpu as pltpu
from jax.sharding import PartitionSpec as P

MESH = pl.DeviceIdType.MESH
AXES = ("gx", "gy", "gz")
EPSILON = 1e-05
BF = jnp.bfloat16
F32 = jnp.float32
PITCH = 48
FIRST = 8


def kernel(
    sizes,
    dims,
    feats,
    ntype,
    bcode,
    wflag,
    ttab,
    btab,
    eself,
    enbr,
    ebias,
    eout,
    nself,
    nagg,
    nout,
    ngain,
    out_lat,
    out_wall,
    lat,
    selfp,
    sb,
    sz,
    hs,
    flag_t,
    zsend,
    zrecv,
    w_sn,
    w_pre,
    w_out,
    bias,
    wall,
    red,
    in_sem,
    out_sem,
    send_sem,
    recv_sem,
    rsend_sem,
    rrecv_sem,
):
    nx, ny, nz, h = dims
    gx, gy, gz = (lax.axis_index(a) for a in AXES)
    here = {"gx": gx, "gy": gy, "gz": gz}

    load = pltpu.make_async_copy(feats, lat, in_sem)
    load.start()
    barrier = pltpu.get_barrier_semaphore()
    peers = 0
    for a in AXES:
        for k in range(1, sizes[a]):
            pl.semaphore_signal(
                barrier,
                inc=1,
                device_id={a: lax.rem(here[a] + k, sizes[a])},
                device_id_type=MESH,
            )
            peers += 1

    for l in range(2):
        w_sn[l, :, :h] = (eself[l].astype(F32) * 0.5).astype(BF)
        w_sn[l, :, h:] = (enbr[l].astype(F32) * 0.5).astype(BF)
        w_pre[l, :h, :] = (nself[l].astype(F32) * 0.5).astype(BF)
        folded = jnp.dot(eout[l], nagg[l], preferred_element_type=F32)
        w_pre[l, h:, :] = (folded * 0.5).astype(BF)
        w = nout[l].astype(F32)
        w_out[l] = (w - jnp.mean(w, axis=1, keepdims=True)).astype(BF)
        for d in range(6):
            row = ebias[l, d : d + 1, :] * 0.5
            bias[l, d] = jnp.broadcast_to(row, (nz, h)).astype(BF)
    wall[...] = jnp.zeros_like(wall)
    zero = jnp.zeros((nx, 1, nz, h), BF)

    @pl.when(gy == 0)
    def _():
        sb[0, 1 : nx + 1, 0:1] = zero
        sb[1, 1 : nx + 1, 0:1] = zero

    @pl.when(gy == sizes["gy"] - 1)
    def _():
        sb[0, 1 : nx + 1, ny + 1 : ny + 2] = zero
        sb[1, 1 : nx + 1, ny + 1 : ny + 2] = zero

    def store_parts(r, x0, cx, y0, cy, both):
        s = both[:, h:].reshape(cx, cy, nz, h)
        selfp[pl.ds(x0, cx), pl.ds(y0, cy)] = both[:, :h].astype(BF).reshape(cx, cy, nz, h)
        sb[r, pl.ds(x0 + 1, cx), pl.ds(y0 + 1, cy)] = s.astype(BF)
        sz[r, pl.ds(x0, cx), pl.ds(y0, cy), FIRST : FIRST + nz, :] = s

    load.wait()

    @pl.loop(0, nx)
    def _(x):
        code = (ntype[x] + 4 * bcode[x]).astype(F32).T
        flag_t[x] = wflag[x].astype(F32).T
        for y in range(ny):
            c = jnp.broadcast_to(code[:, y : y + 1], (nz, h))
            which = c
            extra = jnp.broadcast_to(btab[0:1, :], (nz, h))
            for b in range(1, 3):
                hit = c >= 4.0 * b
                extra = jnp.where(hit, btab[b : b + 1, :], extra)
                which = jnp.where(hit, c - 4.0 * b, which)
            kind = jnp.broadcast_to(ttab[0:1, :], (nz, h))
            for t in range(1, 4):
                kind = jnp.where(which >= 1.0 * t, ttab[t : t + 1, :], kind)
            lat[x, y] = (lat[x, y].astype(F32) + kind + extra).astype(BF)
        both = jnp.dot(
            lat[x].reshape(ny * nz, h), w_sn[0], preferred_element_type=F32
        )
        store_parts(0, x, 1, 0, ny, both)

    def copies(r):
        up = {a: lax.rem(here[a] + 1, sizes[a]) for a in AXES}
        down = {a: lax.rem(here[a] + sizes[a] - 1, sizes[a]) for a in AXES}
        own = lambda f, *at: f.at[(r,) + at]
        rows_x, rows_y = pl.ds(1, nx), pl.ds(1, ny)
        plans = (
            ("gx", up, own(sb, nx, rows_y), own(sb, 0, rows_y)),
            ("gx", down, own(sb, 1, rows_y), own(sb, nx + 1, rows_y)),
            ("gy", up, own(sb, rows_x, ny), own(sb, rows_x, 0)),
            ("gy", down, own(sb, rows_x, 1), own(sb, rows_x, ny + 1)),
            ("gz", up, own(zsend, 1), own(zrecv, 0)),
            ("gz", down, own(zsend, 0), own(zrecv, 1)),
        )
        return [
            pltpu.make_async_remote_copy(
                src_ref=src,
                dst_ref=dst,
                send_sem=send_sem.at[r, k],
                recv_sem=recv_sem.at[r, k],
                device_id={a: to[a]},
                device_id_type=MESH,
            )
            for k, (a, to, src, dst) in enumerate(plans)
        ]

    not_top, not_bottom = gy < sizes["gy"] - 1, gy > 0

    def start_all(r):
        zsend[r, 0] = sz[r, :, :, FIRST, :].astype(BF)
        zsend[r, 1] = sz[r, :, :, FIRST + nz - 1, :].astype(BF)
        both = copies(r)

        @pl.when(not_top)
        def _():
            both[2].start()

        @pl.when(not_bottom)
        def _():
            both[3].start()

        for k in (0, 1, 4, 5):
            both[k].start()
        return both

    def wait_z(r, both):
        both[4].wait_recv()
        both[5].wait_recv()
        sz[r, :, :, FIRST - 1, :] = zrecv[r, 0].astype(F32)
        sz[r, :, :, FIRST + nz, :] = zrecv[r, 1].astype(F32)

    def wait_x(both):
        both[0].wait_recv()
        both[1].wait_recv()

    def wait_y(both):
        @pl.when(not_bottom)
        def _():
            both[2].wait_recv()

        @pl.when(not_top)
        def _():
            both[3].wait_recv()

    def wait_sent(both):
        for k in (0, 1, 4, 5):
            both[k].wait_send()

        @pl.when(not_top)
        def _():
            both[2].wait_send()

        @pl.when(not_bottom)
        def _():
            both[3].wait_send()

    keep_low = jnp.full((nz, h), not_bottom.astype(F32)).astype(BF)
    keep_high = jnp.full((nz, h), not_top.astype(F32)).astype(BF)
    one = jnp.ones((nz, h), BF)

    def block(l, x0, cx, y0, cy):
        for i in range(cx):
            for j in range(cy):
                x, y = x0 + i, y0 + j
                base = selfp[x, y]
                near = (
                    sb[l, x, y + 1],
                    sb[l, x + 2, y + 1],
                    sb[l, x + 1, y],
                    sb[l, x + 1, y + 2],
                    sz[l, x, y, FIRST - 1 : FIRST - 1 + nz, :].astype(BF),
                    sz[l, x, y, FIRST + 1 : FIRST + 1 + nz, :].astype(BF),
                )
                total = None
                for d in range(6):
                    u = (base + bias[l, d]) + near[d]
                    term = u * (one + jnp.tanh(u))
                    if d == 2 and y == 0:
                        term = term * keep_low
                    if d == 3 and y == ny - 1:
                        term = term * keep_high
                    total = term if total is None else total + term
                hs[x, y] = total
        rows = cx * cy * nz
        at = (pl.ds(x0, cx), pl.ds(y0, cy))
        old = lat[at].reshape(rows, h)
        pair = jnp.concatenate([old, hs[at].reshape(rows, h)], axis=1)
        p = jnp.dot(pair, w_pre[l], preferred_element_type=F32).astype(BF)
        inner = p * (jnp.ones_like(p) + jnp.tanh(p))
        update = jnp.dot(inner, w_out[l], preferred_element_type=F32)
        spread = jnp.mean(update * update, axis=1, keepdims=True)
        normed = update * lax.rsqrt(spread + EPSILON) * ngain[l : l + 1, :]
        new = (old.astype(F32) + normed).astype(BF)
        if l == 0:
            lat[at] = new.reshape(cx, cy, nz, h)
            store_parts(1, x0, cx, y0, cy, jnp.dot(new, w_sn[1], preferred_element_type=F32))
        else:
            out_lat[at] = new.reshape(cx, cy, nz, h)
            wide = new.astype(F32).reshape(cx, cy, nz, h)
            for i in range(cx):
                for j in range(cy):
                    flag = flag_t[x0 + i][:, y0 + j : y0 + j + 1]
                    wall[...] += flag * wide[i, j]

    pl.semaphore_wait(barrier, peers)
    for l in range(2):
        both = start_all(l)
        wait_z(l, both)

        @pl.loop(1, nx - 1)
        def _(x):
            block(l, x, 1, 1, ny - 2)

        wait_x(both)

        @pl.loop(0, 2)
        def _(k):
            block(l, k * (nx - 1), 1, 1, ny - 2)

        wait_y(both)
        block(l, 0, nx, 0, 1)
        block(l, 0, nx, ny - 1, 1)
        wait_sent(both)

    red[0, 0, 0:1, :] = jnp.sum(wall[...], axis=0, keepdims=True)
    count = jnp.sum(jnp.sum(jnp.sum(flag_t[...], axis=0), axis=0, keepdims=True), axis=1, keepdims=True)
    red[0, 0, 1:2, :] = jnp.broadcast_to(count, (1, h))
    red[0, 0, 2:8, :] = jnp.zeros((6, h), F32)
    mine = red[0, 0]
    for stage, a in ((0, "gz"), (1, "gy"), (2, "gx")):
        n = sizes[a]
        red[stage + 1, pl.ds(here[a], 1)] = mine[None]
        sent = []
        for k in range(1, n):
            to = lax.rem(here[a] + k, n)
            sent.append(
                pltpu.make_async_remote_copy(
                    src_ref=red.at[stage + 1, here[a]],
                    dst_ref=red.at[stage + 1, here[a]],
                    send_sem=rsend_sem.at[stage, k],
                    recv_sem=rrecv_sem.at[stage, k],
                    device_id={a: to},
                    device_id_type=MESH,
                )
            )
            sent[-1].start()
        for s in sent:
            s.wait()
        mine = red[stage + 1, 0]
        for k in range(1, n):
            mine = mine + red[stage + 1, k]
    out_wall[...] = mine[0:1, :] / mine[1:2, :]


def solution(mesh):
    sizes = {a: mesh.shape[a] for a in AXES}

    def per_device(*args):
        nx, ny, nz, h = dims = args[0].shape
        vmem = pl.BlockSpec(memory_space=pltpu.VMEM)
        latent, mean = pl.pallas_call(
            functools.partial(kernel, sizes, dims),
            out_shape=(
                jax.ShapeDtypeStruct(dims, BF),
                jax.ShapeDtypeStruct((1, h), F32),
            ),
            in_specs=[pl.BlockSpec(memory_space=pl.ANY)] + [vmem] * 13,
            out_specs=(vmem, vmem),
            scratch_shapes=[
                pltpu.VMEM(dims, BF),
                pltpu.VMEM(dims, BF),
                pltpu.VMEM((2, nx + 2, ny + 2, nz, h), BF),
                pltpu.VMEM((2, nx, ny, PITCH, h), F32),
                pltpu.VMEM(dims, BF),
                pltpu.VMEM((nx, nz, ny), F32),
                pltpu.VMEM((2, 2, nx, ny, h), BF),
                pltpu.VMEM((2, 2, nx, ny, h), BF),
                pltpu.VMEM((2, h, 2 * h), BF),
                pltpu.VMEM((2, 2 * h, h), BF),
                pltpu.VMEM((2, h, h), BF),
                pltpu.VMEM((2, 6, nz, h), BF),
                pltpu.VMEM((nz, h), F32),
                pltpu.VMEM((4, 8, 8, h), F32),
                pltpu.SemaphoreType.DMA,
                pltpu.SemaphoreType.DMA,
                pltpu.SemaphoreType.DMA((2, 6)),
                pltpu.SemaphoreType.DMA((2, 6)),
                pltpu.SemaphoreType.DMA((3, 8)),
                pltpu.SemaphoreType.DMA((3, 8)),
            ],
            compiler_params=pltpu.CompilerParams(
                collective_id=0, has_side_effects=True, vmem_limit_bytes=48 * 1024 * 1024
            ),
            name="mesh_step",
        )(*args)
        return latent, mean[0]

    block4 = P(*AXES, None)
    block3 = P(*AXES)
    return jax.shard_map(
        per_device,
        mesh=mesh,
        in_specs=(block4, block3, block3, block3) + (P(),) * 10,
        out_specs=(block4, P()),
        check_vma=False,
    )
```

```python
import functools

import jax
import jax.numpy as jnp
from jax import lax
from jax.experimental import pallas as pl
from jax.experimental.pallas import tpu as pltpu
from jax.sharding import PartitionSpec as P

MESH = pl.DeviceIdType.MESH
AXES = ("gx", "gy", "gz")
EPSILON = 1e-05
BF = jnp.bfloat16
F32 = jnp.float32
PITCH = 48
FIRST = 8
PARTS = 4
CODES = 16


def matmul(a, b):
    return jnp.dot(a, b, preferred_element_type=F32)


def silu_of_double(u):
    return u * (jnp.ones_like(u) + jnp.tanh(u))


def kernel(sizes, dims, *refs):
    hbm, (out_lat, out_wall), vmem, rest = refs[:14], refs[14:16], refs[16:29], refs[29:]
    pl.run_scoped(
        functools.partial(body, sizes, dims, hbm, out_lat, out_wall, vmem, rest),
        *scoped(dims),
    )


def scoped(dims):
    nx, ny, nz, h = dims
    wide = (nx + 2, ny + 2, nz, h)
    return [
        pltpu.VMEM(s, BF)
        for s in (
            dims,
            dims,
            dims,
            wide,
            wide,
            dims,
            dims,
            (2, 2, nx, ny, h),
            (2, 2, nx, ny, h),
            (2, h, 2 * h),
            (2, 2 * h, h),
            (2, h, h),
            (2, 6, nz, h),
            (2 * CODES, 2 * h),
        )
    ]


def body(sizes, dims, hbm, out_lat, out_wall, vmem, rest, *bufs):
    (lat, self0, self1, sb0, sb1, hs, mask, zsend, zrecv, w_sn, w_pre, w_out, bias, tables) = bufs
    (sz0, sz1, flat, wall, line, plane, in_sem, send_sem, recv_sem, rsend_sem, rrecv_sem) = rest
    (ntype, bcode, wflag, ttab, btab, eself, enbr, ebias, eout, nself, nagg, nout, ngain) = vmem
    selfs, sbs, szs = (self0, self1), (sb0, sb1), (sz0, sz1)
    nx, ny, nz, h = dims
    here = {a: lax.axis_index(a) for a in AXES}
    gy = here["gy"]
    not_top, not_bottom = gy < sizes["gy"] - 1, gy > 0

    loads = [
        pltpu.make_async_copy(src, dst, in_sem.at[k])
        for k, (src, dst) in enumerate(zip(hbm, (lat,) + vmem, strict=True))
    ]
    for k in (1, 2, 3, 4, 5, 0, 6, 7, 8, 9, 10, 11, 12, 13):
        loads[k].start()

    barrier = pltpu.get_barrier_semaphore()
    planes = sizes["gx"] * sizes["gy"]
    peers = [{"gz": lax.rem(here["gz"] + k, sizes["gz"])} for k in range(1, sizes["gz"])]
    for k in range(1, planes):
        j = lax.rem(here["gx"] * sizes["gy"] + here["gy"] + k, planes)
        peers.append({"gx": lax.div(j, sizes["gy"]), "gy": lax.rem(j, sizes["gy"])})
    for peer in peers:
        pl.semaphore_signal(barrier, inc=1, device_id=peer, device_id_type=MESH)

    wall[...] = jnp.zeros_like(wall)

    def exchange(slots, spot, n, place, stage):
        sent = []
        for k in range(1, n):
            sent.append(
                pltpu.make_async_remote_copy(
                    src_ref=slots.at[spot],
                    dst_ref=slots.at[spot],
                    send_sem=rsend_sem.at[stage, k],
                    recv_sem=rrecv_sem.at[stage, k],
                    device_id=place(lax.rem(spot + k, n)),
                    device_id_type=MESH,
                )
            )
            sent[-1].start()
        return sent

    def total_of(sent, slots, n):
        for s in sent:
            s.wait()
        total = slots[0]
        for k in range(1, n):
            total = total + slots[k]
        return total

    @pl.when(gy == 0)
    def _():
        @pl.loop(1, nx + 1)
        def _(x):
            sb0[x, 0] = jnp.zeros((nz, h), BF)
            sb1[x, 0] = jnp.zeros((nz, h), BF)

    @pl.when(gy == sizes["gy"] - 1)
    def _():
        @pl.loop(1, nx + 1)
        def _(x):
            sb0[x, ny + 1] = jnp.zeros((nz, h), BF)
            sb1[x, ny + 1] = jnp.zeros((nz, h), BF)

    for k in range(1, 6):
        loads[k].wait()

    columns, per_row = nx * ny, h // nz
    code = (ntype[...] + 4 * bcode[...] + CODES * wflag[...]).astype(F32)
    code = code.reshape(columns, nz).astype(BF)
    iota = lambda shape, d: lax.broadcasted_iota(jnp.int32, shape, d)
    ones_where = lambda hit: jnp.where(hit, 1.0, 0.0)
    repeat = ones_where(lax.rem(iota((nz, h), 1), nz) == iota((nz, h), 0)).astype(BF)
    spread_out = matmul(code, repeat)
    mine = lax.rem(iota((columns, h), 0), per_row) == lax.div(iota((columns, h), 1), nz)
    spread_out = jnp.where(mine, spread_out, 0.0).astype(BF)
    blocks = columns // per_row
    gather = ones_where(
        lax.div(iota((blocks, columns), 1), per_row) == iota((blocks, columns), 0)
    ).astype(BF)
    flat[...] = matmul(gather, spread_out)
    flags = ones_where(flat[...] >= CODES)
    count = jnp.sum(jnp.sum(flags, axis=0, keepdims=True), axis=1, keepdims=True)
    line[pl.ds(here["gz"], 1), 1:2, :] = jnp.broadcast_to(count, (1, h))[None]

    sums = jnp.concatenate(
        [ttab[...] + btab[b : b + 1, :] for b in range(3)] + [jnp.zeros((4, h), F32)], axis=0
    )
    high = sums.astype(BF)
    low = (sums - high.astype(F32)).astype(BF)
    tables[0:CODES, :h] = high
    tables[CODES : 2 * CODES, :h] = low
    last = iota((2 * CODES, h), 0) == 2 * CODES - 1
    tables[:, h:] = ones_where(last).astype(BF)

    for k in range(6, 14):
        loads[k].wait()
    for l in range(2):
        w_sn[l, :, :h] = (eself[l].astype(F32) * 0.5).astype(BF)
        w_sn[l, :, h:] = (enbr[l].astype(F32) * 0.5).astype(BF)
        w_pre[l, :h, :] = (nself[l].astype(F32) * 0.5).astype(BF)
        w_pre[l, h:, :] = (matmul(eout[l], nagg[l]) * 0.5).astype(BF)
        w = nout[l].astype(F32)
        w_out[l] = (w - jnp.mean(w, axis=1, keepdims=True)).astype(BF)
        for d in range(6):
            row = ebias[d, l : l + 1, :] * 0.5
            bias[l, d] = jnp.broadcast_to(row, (nz, h)).astype(BF)

    loads[0].wait()
    per_x = ny // per_row

    def begin(x):
        nodes = ny * nz
        rows = [flat[pl.ds(x * per_x + k, 1), :] for k in range(per_x)]
        nodes_code = jnp.broadcast_to(jnp.concatenate(rows, axis=1), (2 * CODES, nodes))
        on_wall = nodes_code >= CODES
        kind = jnp.where(on_wall, nodes_code - CODES, nodes_code)
        at = iota((2 * CODES, nodes), 0)
        hit = kind == lax.rem(at, CODES).astype(F32)
        hot = jnp.where(at == 2 * CODES - 1, ones_where(on_wall), ones_where(hit)).astype(BF)
        found = lax.dot_general(
            hot, tables[...], (((0,), (0,)), ((), ())), preferred_element_type=F32
        )
        new = (lat[x].reshape(nodes, h).astype(F32) + found[:, :h]).astype(BF)
        return new, found[:, h:].astype(BF), matmul(new, w_sn[0])

    def store_parts(r, at, shape, both):
        x, y = at
        s = both[:, h:].reshape(shape)
        selfs[r][x, y] = both[:, :h].astype(BF).reshape(shape)
        sbs[r][shift(x), shift(y)] = s.astype(BF)
        szs[r][x, y, FIRST : FIRST + nz, :] = s

    def shift(i):
        return pl.ds(i.start + 1, i.size) if isinstance(i, pl.Slice) else i + 1

    with jax.named_scope("prologue"):

        @pl.loop(0, nx // 2)
        def _(i):
            xs = (2 * i, 2 * i + 1)
            results = [begin(x) for x in xs]
            for x, (new, walls, both) in zip(xs, results, strict=True):
                lat[x] = new.reshape(ny, nz, h)
                mask[x] = walls.reshape(ny, nz, h)
                store_parts(0, (x, pl.ds(0, ny)), (ny, nz, h), both)

    def copies(r):
        up = {a: lax.rem(here[a] + 1, sizes[a]) for a in AXES}
        down = {a: lax.rem(here[a] + sizes[a] - 1, sizes[a]) for a in AXES}
        sb = sbs[r]
        rows_x, rows_y = pl.ds(1, nx), pl.ds(1, ny)
        plans = (
            ("gx", up, sb.at[nx, rows_y], sb.at[0, rows_y]),
            ("gx", down, sb.at[1, rows_y], sb.at[nx + 1, rows_y]),
            ("gy", up, sb.at[rows_x, ny], sb.at[rows_x, 0]),
            ("gy", down, sb.at[rows_x, 1], sb.at[rows_x, ny + 1]),
            ("gz", up, zsend.at[r, 1], zrecv.at[r, 0]),
            ("gz", down, zsend.at[r, 0], zrecv.at[r, 1]),
        )
        return [
            pltpu.make_async_remote_copy(
                src_ref=src,
                dst_ref=dst,
                send_sem=send_sem.at[r, k],
                recv_sem=recv_sem.at[r, k],
                device_id={a: to[a]},
                device_id_type=MESH,
            )
            for k, (a, to, src, dst) in enumerate(plans)
        ]

    def start_all(r):
        both = copies(r)
        for k in (0, 1):
            both[k].start()

        @pl.when(not_top)
        def _():
            both[2].start()

        @pl.when(not_bottom)
        def _():
            both[3].start()

        zsend[r, 0] = szs[r][:, :, FIRST, :].astype(BF)
        zsend[r, 1] = szs[r][:, :, FIRST + nz - 1, :].astype(BF)
        for k in (4, 5):
            both[k].start()
        return both

    def wait_z(r, both):
        both[4].wait_recv()
        both[5].wait_recv()
        szs[r][:, :, FIRST - 1, :] = zrecv[r, 0].astype(F32)
        szs[r][:, :, FIRST + nz, :] = zrecv[r, 1].astype(F32)

    def wait_x(both):
        both[0].wait_recv()
        both[1].wait_recv()

    def wait_y(both):
        @pl.when(not_bottom)
        def _():
            both[2].wait_recv()

        @pl.when(not_top)
        def _():
            both[3].wait_recv()

    def wait_sent(both):
        for k in (0, 1, 4, 5):
            both[k].wait_send()

        @pl.when(not_top)
        def _():
            both[2].wait_send()

        @pl.when(not_bottom)
        def _():
            both[3].wait_send()

    def edges(l, x, y, dirs, total):
        base = selfs[l][x, y]
        for d in dirs:
            if d < 4:
                near = sbs[l][x + (0, 2, 1, 1)[d], y + (1, 1, 0, 2)[d]]
            else:
                first = FIRST + (-1, 1)[d - 4]
                near = szs[l][x, y, first : first + nz, :].astype(BF)
            term = silu_of_double((base + bias[l, d]) + near)
            if d == 2 and y == 0:
                term = term * keep(not_bottom)
            if d == 3 and y == ny - 1:
                term = term * keep(not_top)
            total = term if total is None else total + term
        return total

    def keep(cond):
        return jnp.full((nz, h), cond.astype(F32)).astype(BF)

    inner_y = range(1, ny - 1)

    def edges_xy(l, x):
        for y in inner_y:
            hs[x, y] = edges(l, x, y, (0, 1, 2, 3), None)

    def edges_z(l, xs):
        sums = [(x, y, edges(l, x, y, (4, 5), hs[x, y])) for x in xs for y in inner_y]
        for x, y, total in sums:
            hs[x, y] = total

    def node(l, ats, shape):
        rows = 1
        for s in shape[:-1]:
            rows *= s
        take = lambda ref: jnp.concatenate([ref[at].reshape(rows, h) for at in ats], axis=0)
        old = take(lat)
        p = matmul(jnp.concatenate([old, take(hs)], axis=1), w_pre[l]).astype(BF)
        update = matmul(silu_of_double(p), w_out[l])
        spread = jnp.mean(update * update, axis=1, keepdims=True)
        normed = update * lax.rsqrt(spread + EPSILON) * ngain[l : l + 1, :]
        new = (old.astype(F32) + normed).astype(BF)
        part = lambda v, k: v[k * rows : (k + 1) * rows]
        if l == 0:
            both = matmul(new, w_sn[1])
            for k, at in enumerate(ats):
                lat[at] = part(new, k).reshape(shape)
                store_parts(1, at, shape, part(both, k))
        else:
            on_wall = (new * take(mask)).astype(F32)
            wall[...] += jnp.sum(on_wall.reshape(-1, 8, h), axis=0)
            for k, at in enumerate(ats):
                lat[at] = part(new, k).reshape(shape)

    def pair(i):
        face = i == nx // 2 - 1
        return jnp.where(face, 0, 2 * i + 1), jnp.where(face, nx - 1, 2 * i + 2)

    def node_pair(l, i):
        node(l, [(x, pl.ds(1, ny - 2)) for x in pair(i)], (ny - 2, nz, h))

    with jax.named_scope("bar"):
        pl.semaphore_wait(barrier, len(peers))
    for l in range(2):
        with jax.named_scope(f"start{l}"):
            both = start_all(l)
        with jax.named_scope(f"pre{l}"):

            @pl.loop(1, nx - 1)
            def _(x):
                edges_xy(l, x)

        with jax.named_scope(f"waitz{l}"):
            wait_z(l, both)
        with jax.named_scope(f"main{l}"):
            edges_z(l, pair(0))

            @pl.loop(1, nx // 2)
            def _(i):
                @pl.when(i == nx // 2 - 1)
                def _():
                    with jax.named_scope(f"waitx{l}"):
                        wait_x(both)

                    @pl.loop(0, 2)
                    def _(k):
                        edges_xy(l, k * (nx - 1))

                node_pair(l, i - 1)
                edges_z(l, pair(i))

        with jax.named_scope(f"waity{l}"):
            wait_y(both)
        with jax.named_scope(f"by{l}"):
            node_pair(l, nx // 2 - 1)
            for y in (0, ny - 1):

                @pl.loop(0, nx, unroll=4)
                def _(x):
                    hs[x, y] = edges(l, x, y, range(6), None)

            node(l, [(pl.ds(0, nx), 0), (pl.ds(0, nx), ny - 1)], (nx, nz, h))
        with jax.named_scope(f"waits{l}"):
            wait_sent(both)

    leave = pltpu.make_async_copy(lat, out_lat, in_sem.at[0])
    leave.start()
    with jax.named_scope("allred"):
        line[pl.ds(here["gz"], 1), 0:1, :] = jnp.sum(wall[...], axis=0, keepdims=True)[None]
        sent = exchange(line, here["gz"], sizes["gz"], lambda j: {"gz": j}, 0)
        total = total_of(sent, line, sizes["gz"])
        spot = here["gx"] * sizes["gy"] + here["gy"]
        plane[pl.ds(spot, 1)] = total[None]
        place = lambda j: {"gx": lax.div(j, sizes["gy"]), "gy": lax.rem(j, sizes["gy"])}
        sent = exchange(plane, spot, sizes["gx"] * sizes["gy"], place, 1)
        total = total_of(sent, plane, sizes["gx"] * sizes["gy"])
        out_wall[...] = total[0:1, :] / total[1:2, :]
    leave.wait()


def hand_over(latent, mean, out_latent, out_mean, held, held_mean, in_sem, out_sem):
    step = latent.shape[0] // PARTS
    parts = [pl.ds(k * step, step) for k in range(PARTS)]
    ways = [(latent.at[p], held.at[p], out_latent.at[p]) for p in parts]
    ways.append((mean, held_mean, out_mean))
    comes = [pltpu.make_async_copy(w[0], w[1], in_sem.at[k]) for k, w in enumerate(ways)]
    goes = [pltpu.make_async_copy(w[1], w[2], out_sem.at[k]) for k, w in enumerate(ways)]
    for c in comes:
        c.start()
    for c, g in zip(comes, goes, strict=True):
        c.wait()
        g.start()
    for g in goes:
        g.wait()


def solution(mesh):
    sizes = {a: mesh.shape[a] for a in AXES}

    def per_device(*args):
        args = list(args)
        args[8] = jnp.transpose(args[8], (1, 0, 2))
        nx, ny, nz, h = dims = args[0].shape
        hbm = pl.BlockSpec(memory_space=pltpu.HBM)
        vmem = pl.BlockSpec(memory_space=pltpu.VMEM)
        latent, mean = pl.pallas_call(
            functools.partial(kernel, sizes, dims),
            out_shape=(
                jax.ShapeDtypeStruct(dims, BF),
                jax.ShapeDtypeStruct((1, h), F32),
            ),
            in_specs=[hbm] * 14,
            out_specs=(hbm, vmem),
            scratch_shapes=[pltpu.VMEM(a.shape, a.dtype) for a in args[1:]]
            + [
                pltpu.VMEM((nx, ny, PITCH, h), F32),
                pltpu.VMEM((nx, ny, PITCH, h), F32),
                pltpu.VMEM((nx * ny * nz // h, h), F32),
                pltpu.VMEM((8, h), F32),
                pltpu.VMEM((sizes["gz"], 2, h), F32),
                pltpu.VMEM((sizes["gx"] * sizes["gy"], 2, h), F32),
                pltpu.SemaphoreType.DMA((14,)),
                pltpu.SemaphoreType.DMA((2, 6)),
                pltpu.SemaphoreType.DMA((2, 6)),
                pltpu.SemaphoreType.DMA((2, 32)),
                pltpu.SemaphoreType.DMA((2, 32)),
            ],
            compiler_params=pltpu.CompilerParams(
                collective_id=0, has_side_effects=True, vmem_limit_bytes=58 * 1024 * 1024
            ),
            name="mesh_step",
        )(*args)
        latent, mean = pl.pallas_call(
            hand_over,
            out_shape=(
                jax.ShapeDtypeStruct(dims, BF),
                jax.ShapeDtypeStruct((1, h), F32),
            ),
            in_specs=[hbm, hbm],
            out_specs=(hbm, hbm),
            scratch_shapes=[
                pltpu.VMEM(dims, BF),
                pltpu.VMEM((1, h), F32),
                pltpu.SemaphoreType.DMA((PARTS + 1,)),
                pltpu.SemaphoreType.DMA((PARTS + 1,)),
            ],
            compiler_params=pltpu.CompilerParams(vmem_limit_bytes=58 * 1024 * 1024),
            name="hand_over",
        )(latent, mean)
        return latent, mean[0]

    block4 = P(*AXES, None)
    block3 = P(*AXES)
    return jax.shard_map(
        per_device,
        mesh=mesh,
        in_specs=(block4, block3, block3, block3) + (P(),) * 10,
        out_specs=(block4, P()),
        check_vma=False,
    )
```

```python
import functools

import jax
import jax.numpy as jnp
from jax import lax
from jax.experimental import pallas as pl
from jax.experimental.pallas import tpu as pltpu
from jax.sharding import PartitionSpec as P

MESH = pl.DeviceIdType.MESH
AXES = ("gx", "gy", "gz")
EPSILON = 1e-05
BF = jnp.bfloat16
F32 = jnp.float32
PITCH = 48
FIRST = 8
PARTS = 4
SPARE = 3
CODES = 16


def matmul(a, b):
    return jnp.dot(a, b, preferred_element_type=F32)


def silu_of_double(u):
    return u * (jnp.ones_like(u) + jnp.tanh(u))


def kernel(sizes, dims, *refs):
    hbm, (out_lat, out_wall), vmem, rest = refs[:14], refs[14:16], refs[16:29], refs[29:]
    pl.run_scoped(
        functools.partial(body, sizes, dims, hbm, out_lat, out_wall, vmem, rest),
        *scoped(dims),
    )


def scoped(dims):
    nx, ny, nz, h = dims
    more = (nx + SPARE, ny, nz, h)
    wide = (nx + SPARE + 1, ny + 2, nz, h)
    return [
        pltpu.VMEM(s, BF)
        for s in (
            more,
            more,
            more,
            wide,
            wide,
            more,
            more,
            (2, 2, nx, ny, h),
            (2, 2, nx, ny, h),
            (2, h, 2 * h),
            (2, 2 * h, h),
            (2, h, h),
            (2, 6, nz, h),
            (2 * CODES, 2 * h),
        )
    ]


def body(sizes, dims, hbm, out_lat, out_wall, vmem, rest, *bufs):
    (lat, self0, self1, sb0, sb1, hs, mask, zsend, zrecv, w_sn, w_pre, w_out, bias, tables) = bufs
    (sz0, sz1, flat, upd, wall, line, plane, in_sem, send_sem, recv_sem, rsend_sem, rrecv_sem) = rest
    (ntype, bcode, wflag, ttab, btab, eself, enbr, ebias, eout, nself, nagg, nout, ngain) = vmem
    selfs, sbs, szs = (self0, self1), (sb0, sb1), (sz0, sz1)
    nx, ny, nz, h = dims
    here = {a: lax.axis_index(a) for a in AXES}
    gy = here["gy"]
    not_top, not_bottom = gy < sizes["gy"] - 1, gy > 0

    loads = [
        pltpu.make_async_copy(src, dst, in_sem.at[k])
        for k, (src, dst) in enumerate(zip(hbm, (lat.at[pl.ds(0, nx)],) + vmem, strict=True))
    ]
    for k in (1, 2, 3, 0, 4, 5, 6, 7, 8, 9, 10, 11, 12, 13):
        loads[k].start()

    barrier = pltpu.get_barrier_semaphore()
    planes = sizes["gx"] * sizes["gy"]
    peers = [{"gz": lax.rem(here["gz"] + k, sizes["gz"])} for k in range(1, sizes["gz"])]
    for k in range(1, planes):
        j = lax.rem(here["gx"] * sizes["gy"] + here["gy"] + k, planes)
        peers.append({"gx": lax.div(j, sizes["gy"]), "gy": lax.rem(j, sizes["gy"])})
    for peer in peers:
        pl.semaphore_signal(barrier, inc=1, device_id=peer, device_id_type=MESH)

    wall[...] = jnp.zeros_like(wall)

    def exchange(slots, spot, n, place, stage):
        def copy(ref, to):
            return pltpu.make_async_remote_copy(
                src_ref=ref,
                dst_ref=ref,
                send_sem=rsend_sem.at[stage],
                recv_sem=rrecv_sem.at[stage],
                device_id=place(to),
                device_id_type=MESH,
            )

        for k in range(1, n):
            copy(slots.at[spot], lax.rem(spot + k, n)).start()
        copy(slots.at[pl.ds(0, n - 1)], lax.rem(spot + 1, n)).wait()
        total = slots[0]
        for k in range(1, n):
            total = total + slots[k]
        return total

    upd[...] = jnp.zeros_like(upd)
    spare = (nx + 1, nx + 2)
    for x in spare:
        for ref in (lat, hs, mask):
            ref[x] = jnp.zeros((ny, nz, h), BF)

    @pl.when(gy == 0)
    def _():
        @pl.loop(1, nx + 1)
        def _(x):
            sb0[x, 0] = jnp.zeros((nz, h), BF)
            sb1[x, 0] = jnp.zeros((nz, h), BF)

    @pl.when(gy == sizes["gy"] - 1)
    def _():
        @pl.loop(1, nx + 1)
        def _(x):
            sb0[x, ny + 1] = jnp.zeros((nz, h), BF)
            sb1[x, ny + 1] = jnp.zeros((nz, h), BF)

    for k in range(1, 6):
        loads[k].wait()

    columns, per_row = nx * ny, h // nz
    code = (ntype[...] + 4 * bcode[...] + CODES * wflag[...]).astype(F32)
    code = code.reshape(columns, nz).astype(BF)
    iota = lambda shape, d: lax.broadcasted_iota(jnp.int32, shape, d)
    ones_where = lambda hit: jnp.where(hit, 1.0, 0.0)
    repeat = ones_where(lax.rem(iota((nz, h), 1), nz) == iota((nz, h), 0)).astype(BF)
    spread_out = matmul(code, repeat)
    turned = lambda y: lax.rem(y + 1, ny)
    slot = lax.rem(turned(lax.rem(iota((columns, h), 0), ny)), per_row)
    spread_out = jnp.where(slot == lax.div(iota((columns, h), 1), nz), spread_out, 0.0).astype(BF)
    per_x = ny // per_row
    blocks = (nx * per_x, columns)
    row, column = iota(blocks, 0), iota(blocks, 1)
    belongs = jnp.logical_and(
        lax.rem(row, nx) == lax.div(column, ny),
        lax.div(row, nx) == lax.div(turned(lax.rem(column, ny)), per_row),
    )
    flat[...] = matmul(ones_where(belongs).astype(BF), spread_out)

    sums = jnp.concatenate(
        [ttab[...] + btab[b : b + 1, :] for b in range(3)] + [jnp.zeros((4, h), F32)], axis=0
    )
    high = sums.astype(BF)
    low = (sums - high.astype(F32)).astype(BF)
    tables[0:CODES, :h] = high
    tables[CODES : 2 * CODES, :h] = low
    last = iota((2 * CODES, h), 0) == 2 * CODES - 1
    tables[:, h:] = ones_where(last).astype(BF)

    def prepare(l):
        w_pre[l, :h, :] = (nself[l].astype(F32) * 0.5).astype(BF)
        w_pre[l, h:, :] = (matmul(eout[l], nagg[l]) * 0.5).astype(BF)
        w = nout[l].astype(F32)
        w_out[l] = (w - jnp.mean(w, axis=1, keepdims=True)).astype(BF)
        for d in range(6):
            row = ebias[d, l : l + 1, :] * 0.5
            bias[l, d] = jnp.broadcast_to(row, (nz, h)).astype(BF)

    for k in range(6, 14):
        loads[k].wait()
    for l in range(2):
        w_sn[l, :, :h] = (eself[l].astype(F32) * 0.5).astype(BF)
        w_sn[l, :, h:] = (enbr[l].astype(F32) * 0.5).astype(BF)
    loads[0].wait()

    for k, z in enumerate((0, nz - 1)):
        kind = jnp.broadcast_to(code[:, z : z + 1].astype(F32), (columns, 2 * CODES))
        kind = jnp.where(kind >= CODES, kind - CODES, kind)
        hot = ones_where(kind == lax.rem(iota((columns, 2 * CODES), 1), CODES).astype(F32))
        found = matmul(hot.astype(BF), tables[:, :h])
        face = lat[0:nx, :, z, :].astype(F32).reshape(columns, h)
        new = (face + found).astype(BF)
        zsend[0, k] = matmul(new, w_sn[0, :, h:]).astype(BF).reshape(nx, ny, h)

    def begin(rows, ats, shapes):
        nodes = len(rows) * h
        nodes_code = jnp.concatenate([flat[pl.ds(r, 1), :] for r in rows], axis=1)
        nodes_code = jnp.broadcast_to(nodes_code, (2 * CODES, nodes))
        on_wall = nodes_code >= CODES
        kind = jnp.where(on_wall, nodes_code - CODES, nodes_code)
        at = iota((2 * CODES, nodes), 0)
        hit = kind == lax.rem(at, CODES).astype(F32)
        hot = jnp.where(at == 2 * CODES - 1, ones_where(on_wall), ones_where(hit)).astype(BF)
        found = lax.dot_general(
            hot, tables[...], (((0,), (0,)), ((), ())), preferred_element_type=F32
        )
        old = jnp.concatenate([lat[at].reshape(-1, h) for at in ats], axis=0)
        new = (old.astype(F32) + found[:, :h]).astype(BF)
        walls = found[:, h:].astype(BF)
        both = matmul(new, w_sn[0])
        first = 0
        for at, shape in zip(ats, shapes, strict=True):
            part = slice(first, first + shape[0] * nz)
            first += shape[0] * nz
            lat[at] = new[part].reshape(shape)
            mask[at] = walls[part].reshape(shape)
            store_parts(0, at, shape, both[part])

    def store_parts(r, at, shape, both):
        x, y = at
        s = both[:, h:].reshape(shape)
        selfs[r][x, y] = both[:, :h].astype(BF).reshape(shape)
        sbs[r][shift(x), shift(y)] = s.astype(BF)
        szs[r][x, y, FIRST : FIRST + nz, :] = s

    def shift(i):
        return pl.ds(i.start + 1, i.size) if isinstance(i, pl.Slice) else i + 1

    def copies(r):
        up = {a: lax.rem(here[a] + 1, sizes[a]) for a in AXES}
        down = {a: lax.rem(here[a] + sizes[a] - 1, sizes[a]) for a in AXES}
        sb = sbs[r]
        rows_x, rows_y = pl.ds(1, nx), pl.ds(1, ny)
        plans = (
            ("gx", up, sb.at[nx, rows_y], sb.at[0, rows_y]),
            ("gx", down, sb.at[1, rows_y], sb.at[nx + 1, rows_y]),
            ("gy", up, sb.at[rows_x, ny], sb.at[rows_x, 0]),
            ("gy", down, sb.at[rows_x, 1], sb.at[rows_x, ny + 1]),
            ("gz", up, zsend.at[r, 1], zrecv.at[r, 0]),
            ("gz", down, zsend.at[r, 0], zrecv.at[r, 1]),
        )
        return [
            pltpu.make_async_remote_copy(
                src_ref=src,
                dst_ref=dst,
                send_sem=send_sem.at[r, k],
                recv_sem=recv_sem.at[r, k],
                device_id={a: to[a]},
                device_id_type=MESH,
            )
            for k, (a, to, src, dst) in enumerate(plans)
        ]

    def start_z(both):
        both[4].start()
        both[5].start()

    def start_x(both):
        both[0].start()
        both[1].start()

    def start_y(both):
        @pl.when(not_top)
        def _():
            both[2].start()

        @pl.when(not_bottom)
        def _():
            both[3].start()

    def wait_z(r, both):
        both[4].wait_recv()
        both[5].wait_recv()
        szs[r][0:nx, :, FIRST - 1, :] = zrecv[r, 0].astype(F32)
        szs[r][0:nx, :, FIRST + nz, :] = zrecv[r, 1].astype(F32)

    def wait_x(both):
        both[0].wait_recv()
        both[1].wait_recv()

    def wait_y(both):
        @pl.when(not_bottom)
        def _():
            both[2].wait_recv()

        @pl.when(not_top)
        def _():
            both[3].wait_recv()

    def wait_sent(both):
        for k in (0, 1, 4, 5):
            both[k].wait_send()

        @pl.when(not_top)
        def _():
            both[2].wait_send()

        @pl.when(not_bottom)
        def _():
            both[3].wait_send()

    def edges(l, x, y, dirs, total):
        base = selfs[l][x, y]
        for d in dirs:
            if d < 4:
                near = sbs[l][x + (0, 2, 1, 1)[d], y + (1, 1, 0, 2)[d]]
            else:
                first = FIRST + (-1, 1)[d - 4]
                near = szs[l][x, y, first : first + nz, :].astype(BF)
            term = silu_of_double((base + bias[l, d]) + near)
            if d == 2 and y == 0:
                term = term * keep(not_bottom)
            if d == 3 and y == ny - 1:
                term = term * keep(not_top)
            total = term if total is None else total + term
        return total

    def keep(cond):
        return jnp.full((nz, h), cond.astype(F32)).astype(BF)

    def take(ref, ats):
        return jnp.concatenate([ref[at].reshape(-1, h) for at in ats], axis=0)

    def update_of(l, old, hidden):
        p = matmul(jnp.concatenate([old, hidden], axis=1), w_pre[l]).astype(BF)
        return matmul(silu_of_double(p), w_out[l])

    def latent_of(l, old, update):
        spread = jnp.mean(update * update, axis=1, keepdims=True)
        normed = update * lax.rsqrt(spread + EPSILON) * ngain[l : l + 1, :]
        return (old.astype(F32) + normed).astype(BF)

    def finish(l, ats, shape, new, walls):
        rows = new.shape[0] // len(ats)
        both = matmul(new, w_sn[1]) if l == 0 else None
        if l == 1:
            wall[...] += jnp.sum((new * walls).astype(F32).reshape(-1, 8, h), axis=0)
        for k, at in enumerate(ats):
            part = slice(k * rows, (k + 1) * rows)
            if l == 0:
                lat[at] = new[part].reshape(shape)
                store_parts(1, at, shape, both[part])
            else:
                out_lat[at] = new[part].reshape(shape)

    face = nx // 2 - 1

    def pair(i):
        if isinstance(i, int):
            return (0, nx - 1) if i == face else (2 * i + 1, 2 * i + 2)
        first = jnp.where(i == face, 0, 2 * i + 1)
        second = jnp.where(i == face, nx - 1, 2 * i + 2)
        return jnp.where(i < 0, spare[0], first), jnp.where(i < 0, spare[1], second)

    inner = pl.ds(1, ny - 2)
    inner_shape = (ny - 2, nz, h)
    inner_rows = 2 * (ny - 2) * nz
    ats_of = lambda i: [(x, inner) for x in pair(i)]
    walls_of = lambda l, ats: take(mask, ats) if l == 1 else None
    y_ats = [(pl.ds(0, nx), 0), (pl.ds(0, nx), ny - 1)]

    travel = [copies(0), copies(1)]
    with jax.named_scope("prologue"):

        @pl.loop(0, 2)
        def _(c):
            half = nx // 2
            xs = [half * c + k for k in range(half)]
            ats, shapes = [], []
            for x in xs:
                ats += [(x, pl.ds(ny - 1, 1)), (x, pl.ds(0, per_row - 1))]
                shapes += [(1, nz, h), (per_row - 1, nz, h)]
            begin(xs, ats, shapes)

        with jax.named_scope("bar"):
            pl.semaphore_wait(barrier, len(peers))
        start_z(travel[0])
        start_y(travel[0])

        @pl.loop(0, nx // 2)
        def _(i):
            xs = (jnp.where(i == 0, 0, 2 * i - 1), jnp.where(i == 0, nx - 1, 2 * i))
            rest = ny - per_row
            rows = [g * nx + x for x in xs for g in range(1, per_x)]
            begin(rows, [(x, pl.ds(per_row - 1, rest)) for x in xs], [(rest, nz, h)] * 2)

            @pl.when(i == 0)
            def _():
                start_x(travel[0])

        prepare(0)

    for l in range(2):
        both = travel[l]
        if l == 1:
            with jax.named_scope("start1"):
                start_y(both)
                start_x(both)
                zsend[1, 0] = sz1[0:nx, :, FIRST, :].astype(BF)
                zsend[1, 1] = sz1[0:nx, :, FIRST + nz - 1, :].astype(BF)
                start_z(both)
                prepare(1)
                flags = ones_where(flat[...] >= CODES)
                count = jnp.sum(jnp.sum(flags, axis=0, keepdims=True), axis=1, keepdims=True)
                line[pl.ds(here["gz"], 1), 1:2, :] = jnp.broadcast_to(count, (1, h))[None]
        with jax.named_scope(f"waitz{l}"):
            wait_z(l, both)
        with jax.named_scope(f"main{l}"):

            @pl.loop(0, nx // 2)
            def _(i):
                @pl.when(i == face)
                def _():
                    with jax.named_scope(f"waitx{l}"):
                        wait_x(both)

                ats_b, ats_c = ats_of(i - 1), ats_of(i - 2)
                update_c, old_c = upd[0:inner_rows, :], take(lat, ats_c)
                old_b, hidden_b, walls_c = take(lat, ats_b), take(hs, ats_b), walls_of(l, ats_c)
                new_c = latent_of(l, old_c, update_c)
                into = ats_c if l == 0 else ats_of(jnp.where(i < 2, face, i - 2))
                finish(l, into, inner_shape, new_c, walls_c)
                update_b = update_of(l, old_b, hidden_b)
                upd[0:inner_rows, :] = update_b
                for x in pair(i):
                    for y in range(1, ny - 1):
                        hs[x, y] = edges(l, x, y, range(6), None)

        with jax.named_scope(f"waity{l}"):
            wait_y(both)
        with jax.named_scope(f"by{l}"):
            ats_b, ats_c = ats_of(face), ats_of(face - 1)
            update_c, old_c = upd[0:inner_rows, :], take(lat, ats_c)
            old_b, hidden_b = take(lat, ats_b), take(hs, ats_b)
            update_b = update_of(l, old_b, hidden_b)
            new_c = latent_of(l, old_c, update_c)
            walls_c, walls_b = walls_of(l, ats_c), walls_of(l, ats_b)
            old_y, walls_y = take(lat, y_ats), walls_of(l, y_ats)
            for y in (0, ny - 1):
                for x in range(nx):
                    hs[x, y] = edges(l, x, y, range(6), None)
            finish(l, ats_c, inner_shape, new_c, walls_c)
            update_y = update_of(l, old_y, take(hs, y_ats))
            finish(l, ats_b, inner_shape, latent_of(l, old_b, update_b), walls_b)
            finish(l, y_ats, (nx, nz, h), latent_of(l, old_y, update_y), walls_y)
        with jax.named_scope(f"waits{l}"):
            wait_sent(both)

    with jax.named_scope("allred"):
        line[pl.ds(here["gz"], 1), 0:1, :] = jnp.sum(wall[...], axis=0, keepdims=True)[None]
        total = exchange(line, here["gz"], sizes["gz"], lambda j: {"gz": j}, 0)
        spot = here["gx"] * sizes["gy"] + here["gy"]
        plane[pl.ds(spot, 1)] = total[None]
        place = lambda j: {"gx": lax.div(j, sizes["gy"]), "gy": lax.rem(j, sizes["gy"])}
        total = exchange(plane, spot, sizes["gx"] * sizes["gy"], place, 1)
        out_wall[...] = total[0:1, :] / total[1:2, :]


def hand_over(latent, mean, out_latent, out_mean, sem):
    step = latent.shape[0] // PARTS
    parts = [pl.ds(k * step, step) for k in range(PARTS)]
    ways = [(mean, out_mean)] + [(latent.at[p], out_latent.at[p]) for p in parts]
    goes = [pltpu.make_async_copy(a, b, sem.at[k]) for k, (a, b) in enumerate(ways)]
    for g in goes:
        g.start()
    for g in goes:
        g.wait()


def solution(mesh):
    sizes = {a: mesh.shape[a] for a in AXES}

    def per_device(*args):
        args = list(args)
        args[8] = jnp.transpose(args[8], (1, 0, 2))
        args = [pltpu.with_memory_space_constraint(a, pltpu.HBM) for a in args]
        nx, ny, nz, h = dims = args[0].shape
        hbm = pl.BlockSpec(memory_space=pltpu.HBM)
        vmem = pl.BlockSpec(memory_space=pltpu.VMEM)
        latent, mean = pl.pallas_call(
            functools.partial(kernel, sizes, dims),
            out_shape=(
                jax.ShapeDtypeStruct(dims, BF),
                jax.ShapeDtypeStruct((1, h), F32),
            ),
            in_specs=[hbm] * 14,
            out_specs=(vmem, vmem),
            scratch_shapes=[pltpu.VMEM(a.shape, a.dtype) for a in args[1:]]
            + [
                pltpu.VMEM((nx + SPARE, ny, PITCH, h), F32),
                pltpu.VMEM((nx + SPARE, ny, PITCH, h), F32),
                pltpu.VMEM((nx * ny * nz // h, h), F32),
                pltpu.VMEM((2 * nx * nz, h), F32),
                pltpu.VMEM((8, h), F32),
                pltpu.VMEM((sizes["gz"], 2, h), F32),
                pltpu.VMEM((sizes["gx"] * sizes["gy"], 2, h), F32),
                pltpu.SemaphoreType.DMA((14,)),
                pltpu.SemaphoreType.DMA((2, 6)),
                pltpu.SemaphoreType.DMA((2, 6)),
                pltpu.SemaphoreType.DMA((2,)),
                pltpu.SemaphoreType.DMA((2,)),
            ],
            compiler_params=pltpu.CompilerParams(
                collective_id=0, has_side_effects=True, vmem_limit_bytes=48 * 1024 * 1024
            ),
            name="mesh_step",
        )(*args)
        latent, mean = pl.pallas_call(
            hand_over,
            out_shape=(
                jax.ShapeDtypeStruct(dims, BF),
                jax.ShapeDtypeStruct((1, h), F32),
            ),
            in_specs=[vmem, vmem],
            out_specs=(hbm, hbm),
            scratch_shapes=[
                pltpu.SemaphoreType.DMA((PARTS + 1,)),
            ],
            compiler_params=pltpu.CompilerParams(vmem_limit_bytes=16 * 1024 * 1024),
            name="hand_over",
        )(latent, mean)
        return latent, mean[0]

    block4 = P(*AXES, None)
    block3 = P(*AXES)
    return jax.shard_map(
        per_device,
        mesh=mesh,
        in_specs=(block4, block3, block3, block3) + (P(),) * 10,
        out_specs=(block4, P()),
        check_vma=False,
    )
```

```python
import functools

import jax
import jax.numpy as jnp
from jax import lax
from jax.experimental import pallas as pl
from jax.experimental.pallas import tpu as pltpu
from jax.sharding import PartitionSpec as P

MESH = pl.DeviceIdType.MESH
AXES = ("gx", "gy", "gz")
EPSILON = 1e-05
BF = jnp.bfloat16
F32 = jnp.float32
PITCH = 48
FIRST = 8
PARTS = 4
SPARE = 3
CODES = 16


def matmul(a, b):
    return jnp.dot(a, b, preferred_element_type=F32)


def silu_of_double(u):
    return u * (jnp.ones_like(u) + jnp.tanh(u))


def kernel(sizes, dims, *refs):
    hbm, (out_lat, out_wall), vmem, rest = refs[:14], refs[14:16], refs[16:29], refs[29:]
    pl.run_scoped(
        functools.partial(body, sizes, dims, hbm, out_lat, out_wall, vmem, rest),
        *scoped(dims),
    )


def scoped(dims):
    nx, ny, nz, h = dims
    more = (nx + SPARE, ny, nz, h)
    wide = (nx + SPARE + 1, ny + 2, nz, h)
    return [
        pltpu.VMEM(s, BF)
        for s in (
            more,
            more,
            more,
            wide,
            wide,
            more,
            more,
            (2, 2, nx, ny, h),
            (2, 2, nx, ny, h),
            (2, h, 2 * h),
            (2, 2 * h, h),
            (2, h, h),
            (2, 6, nz, h),
            (2 * CODES, 2 * h),
        )
    ]


def body(sizes, dims, hbm, out_lat, out_wall, vmem, rest, *bufs):
    (lat, self0, self1, sb0, sb1, hs, mask, zsend, zrecv, w_sn, w_pre, w_out, bias, tables) = bufs
    (sz0, sz1, flat, upd, wall, line, plane, in_sem, send_sem, recv_sem, rsend_sem, rrecv_sem) = rest
    (ntype, bcode, wflag, ttab, btab, eself, enbr, ebias, eout, nself, nagg, nout, ngain) = vmem
    selfs, sbs, szs = (self0, self1), (sb0, sb1), (sz0, sz1)
    nx, ny, nz, h = dims
    here = {a: lax.axis_index(a) for a in AXES}
    gy = here["gy"]
    not_top, not_bottom = gy < sizes["gy"] - 1, gy > 0

    loads = [
        pltpu.make_async_copy(src, dst, in_sem.at[k])
        for k, (src, dst) in enumerate(zip(hbm, (lat.at[pl.ds(0, nx)],) + vmem, strict=True))
    ]
    for k in (1, 2, 3, 0, 4, 5, 6, 7, 8, 9, 10, 11, 12, 13):
        loads[k].start()

    barrier = pltpu.get_barrier_semaphore()
    planes = sizes["gx"] * sizes["gy"]
    peers = [{"gz": lax.rem(here["gz"] + k, sizes["gz"])} for k in range(1, sizes["gz"])]
    for k in range(1, planes):
        j = lax.rem(here["gx"] * sizes["gy"] + here["gy"] + k, planes)
        peers.append({"gx": lax.div(j, sizes["gy"]), "gy": lax.rem(j, sizes["gy"])})
    for peer in peers:
        pl.semaphore_signal(barrier, inc=1, device_id=peer, device_id_type=MESH)

    wall[...] = jnp.zeros_like(wall)

    def exchange(slots, spot, n, place, stage):
        def copy(ref, to):
            return pltpu.make_async_remote_copy(
                src_ref=ref,
                dst_ref=ref,
                send_sem=rsend_sem.at[stage],
                recv_sem=rrecv_sem.at[stage],
                device_id=place(to),
                device_id_type=MESH,
            )

        for k in range(1, n):
            copy(slots.at[spot], lax.rem(spot + k, n)).start()
        copy(slots.at[pl.ds(0, n - 1)], lax.rem(spot + 1, n)).wait()
        total = slots[0]
        for k in range(1, n):
            total = total + slots[k]
        return total

    upd[...] = jnp.zeros_like(upd)
    spare = (nx + 1, nx + 2)
    for x in spare:
        for ref in (lat, hs, mask):
            ref[x] = jnp.zeros((ny, nz, h), BF)

    @pl.when(gy == 0)
    def _():
        @pl.loop(1, nx + 1)
        def _(x):
            sb0[x, 0] = jnp.zeros((nz, h), BF)
            sb1[x, 0] = jnp.zeros((nz, h), BF)

    @pl.when(gy == sizes["gy"] - 1)
    def _():
        @pl.loop(1, nx + 1)
        def _(x):
            sb0[x, ny + 1] = jnp.zeros((nz, h), BF)
            sb1[x, ny + 1] = jnp.zeros((nz, h), BF)

    for k in range(1, 6):
        loads[k].wait()

    columns, per_row = nx * ny, h // nz
    code = (ntype[...] + 4 * bcode[...] + CODES * wflag[...]).astype(F32)
    code = code.reshape(columns, nz).astype(BF)
    iota = lambda shape, d: lax.broadcasted_iota(jnp.int32, shape, d)
    ones_where = lambda hit: jnp.where(hit, 1.0, 0.0)
    repeat = ones_where(lax.rem(iota((nz, h), 1), nz) == iota((nz, h), 0)).astype(BF)
    spread_out = matmul(code, repeat)
    turned = lambda y: lax.rem(y + 1, ny)
    slot = lax.rem(turned(lax.rem(iota((columns, h), 0), ny)), per_row)
    spread_out = jnp.where(slot == lax.div(iota((columns, h), 1), nz), spread_out, 0.0).astype(BF)
    per_x = ny // per_row
    blocks = (nx * per_x, columns)
    row, column = iota(blocks, 0), iota(blocks, 1)
    belongs = jnp.logical_and(
        lax.rem(row, nx) == lax.div(column, ny),
        lax.div(row, nx) == lax.div(turned(lax.rem(column, ny)), per_row),
    )
    flat[...] = matmul(ones_where(belongs).astype(BF), spread_out)

    sums = jnp.concatenate(
        [ttab[...] + btab[b : b + 1, :] for b in range(3)] + [jnp.zeros((4, h), F32)], axis=0
    )
    high = sums.astype(BF)
    low = (sums - high.astype(F32)).astype(BF)
    tables[0:CODES, :h] = high
    tables[CODES : 2 * CODES, :h] = low
    last = iota((2 * CODES, h), 0) == 2 * CODES - 1
    tables[:, h:] = ones_where(last).astype(BF)

    def prepare(l):
        w_pre[l, :h, :] = (nself[l].astype(F32) * 0.5).astype(BF)
        w_pre[l, h:, :] = (matmul(eout[l], nagg[l]) * 0.5).astype(BF)
        w = nout[l].astype(F32)
        w_out[l] = (w - jnp.mean(w, axis=1, keepdims=True)).astype(BF)
        for d in range(6):
            row = ebias[d, l : l + 1, :] * 0.5
            bias[l, d] = jnp.broadcast_to(row, (nz, h)).astype(BF)

    for k in range(6, 14):
        loads[k].wait()
    for l in range(2):
        w_sn[l, :, :h] = (eself[l].astype(F32) * 0.5).astype(BF)
        w_sn[l, :, h:] = (enbr[l].astype(F32) * 0.5).astype(BF)
    loads[0].wait()

    for k, z in enumerate((0, nz - 1)):
        kind = jnp.broadcast_to(code[:, z : z + 1].astype(F32), (columns, 2 * CODES))
        kind = jnp.where(kind >= CODES, kind - CODES, kind)
        hot = ones_where(kind == lax.rem(iota((columns, 2 * CODES), 1), CODES).astype(F32))
        found = matmul(hot.astype(BF), tables[:, :h])
        face = lat[0:nx, :, z, :].astype(F32).reshape(columns, h)
        new = (face + found).astype(BF)
        zsend[0, k] = matmul(new, w_sn[0, :, h:]).astype(BF).reshape(nx, ny, h)

    def take(ref, ats):
        return jnp.concatenate([ref[at].reshape(-1, h) for at in ats], axis=0)

    def look_up(rows, old):
        nodes = len(rows) * h
        nodes_code = jnp.concatenate([flat[pl.ds(r, 1), :] for r in rows], axis=1)
        nodes_code = jnp.broadcast_to(nodes_code, (2 * CODES, nodes))
        on_wall = nodes_code >= CODES
        kind = jnp.where(on_wall, nodes_code - CODES, nodes_code)
        at = iota((2 * CODES, nodes), 0)
        hit = kind == lax.rem(at, CODES).astype(F32)
        hot = jnp.where(at == 2 * CODES - 1, ones_where(on_wall), ones_where(hit)).astype(BF)
        found = lax.dot_general(
            hot, tables[...], (((0,), (0,)), ((), ())), preferred_element_type=F32
        )
        return (old.astype(F32) + found[:, :h]).astype(BF), found[:, h:].astype(BF)

    def pieces(ats, shapes):
        first = 0
        for at, shape in zip(ats, shapes, strict=True):
            yield at, shape, slice(first, first + shape[0] * nz)
            first += shape[0] * nz

    def store_nodes(ats, shapes, new, walls):
        for at, shape, part in pieces(ats, shapes):
            lat[at] = new[part].reshape(shape)
            mask[at] = walls[part].reshape(shape)

    def store_projected(ats, shapes, both):
        for at, shape, part in pieces(ats, shapes):
            store_parts(0, at, shape, both[part])

    def store_parts(r, at, shape, both):
        x, y = at
        s = both[:, h:].reshape(shape)
        selfs[r][x, y] = both[:, :h].astype(BF).reshape(shape)
        sbs[r][shift(x), shift(y)] = s.astype(BF)
        szs[r][x, y, FIRST : FIRST + nz, :] = s

    def shift(i):
        return pl.ds(i.start + 1, i.size) if isinstance(i, pl.Slice) else i + 1

    def copies(r):
        up = {a: lax.rem(here[a] + 1, sizes[a]) for a in AXES}
        down = {a: lax.rem(here[a] + sizes[a] - 1, sizes[a]) for a in AXES}
        sb = sbs[r]
        rows_x, rows_y = pl.ds(1, nx), pl.ds(1, ny)
        plans = (
            ("gx", up, sb.at[nx, rows_y], sb.at[0, rows_y]),
            ("gx", down, sb.at[1, rows_y], sb.at[nx + 1, rows_y]),
            ("gy", up, sb.at[rows_x, ny], sb.at[rows_x, 0]),
            ("gy", down, sb.at[rows_x, 1], sb.at[rows_x, ny + 1]),
            ("gz", up, zsend.at[r, 1], zrecv.at[r, 0]),
            ("gz", down, zsend.at[r, 0], zrecv.at[r, 1]),
        )
        return [
            pltpu.make_async_remote_copy(
                src_ref=src,
                dst_ref=dst,
                send_sem=send_sem.at[r, k],
                recv_sem=recv_sem.at[r, k],
                device_id={a: to[a]},
                device_id_type=MESH,
            )
            for k, (a, to, src, dst) in enumerate(plans)
        ]

    def start_z(both):
        both[4].start()
        both[5].start()

    def start_x(both):
        both[0].start()
        both[1].start()

    def start_y(both):
        @pl.when(not_top)
        def _():
            both[2].start()

        @pl.when(not_bottom)
        def _():
            both[3].start()

    def wait_z(r, both):
        both[4].wait_recv()
        both[5].wait_recv()
        szs[r][0:nx, :, FIRST - 1, :] = zrecv[r, 0].astype(F32)
        szs[r][0:nx, :, FIRST + nz, :] = zrecv[r, 1].astype(F32)

    def wait_x(both):
        both[0].wait_recv()
        both[1].wait_recv()

    def wait_y(both):
        @pl.when(not_bottom)
        def _():
            both[2].wait_recv()

        @pl.when(not_top)
        def _():
            both[3].wait_recv()

    def wait_sent(both):
        for k in (0, 1, 4, 5):
            both[k].wait_send()

        @pl.when(not_top)
        def _():
            both[2].wait_send()

        @pl.when(not_bottom)
        def _():
            both[3].wait_send()

    def edges(l, x, y, dirs, total):
        base = selfs[l][x, y]
        for d in dirs:
            if d < 4:
                near = sbs[l][x + (0, 2, 1, 1)[d], y + (1, 1, 0, 2)[d]]
            else:
                first = FIRST + (-1, 1)[d - 4]
                near = szs[l][x, y, first : first + nz, :].astype(BF)
            term = silu_of_double((base + bias[l, d]) + near)
            if d == 2 and y == 0:
                term = term * keep(not_bottom)
            if d == 3 and y == ny - 1:
                term = term * keep(not_top)
            total = term if total is None else total + term
        return total

    def edges_xy(l, x):
        for y in range(1, ny - 1):
            hs[x, y] = edges(l, x, y, (0, 1, 2, 3), None)

    def keep(cond):
        return jnp.full((nz, h), cond.astype(F32)).astype(BF)

    def update_of(l, old, hidden):
        p = matmul(jnp.concatenate([old, hidden], axis=1), w_pre[l]).astype(BF)
        return matmul(silu_of_double(p), w_out[l])

    def latent_of(l, old, update):
        spread = jnp.mean(update * update, axis=1, keepdims=True)
        normed = update * lax.rsqrt(spread + EPSILON) * ngain[l : l + 1, :]
        return (old.astype(F32) + normed).astype(BF)

    def finish(l, ats, shape, new, walls):
        rows = new.shape[0] // len(ats)
        both = matmul(new, w_sn[1]) if l == 0 else None
        if l == 1:
            wall[...] += jnp.sum((new * walls).astype(F32).reshape(-1, 8, h), axis=0)
        for k, at in enumerate(ats):
            part = slice(k * rows, (k + 1) * rows)
            if l == 0:
                lat[at] = new[part].reshape(shape)
                store_parts(1, at, shape, both[part])
            else:
                out_lat[at] = new[part].reshape(shape)

    face = nx // 2 - 1

    def pair(i):
        if isinstance(i, int):
            return (0, nx - 1) if i == face else (2 * i + 1, 2 * i + 2)
        first = jnp.where(i == face, 0, 2 * i + 1)
        second = jnp.where(i == face, nx - 1, 2 * i + 2)
        return jnp.where(i < 0, spare[0], first), jnp.where(i < 0, spare[1], second)

    inner = pl.ds(1, ny - 2)
    inner_shape = (ny - 2, nz, h)
    inner_rows = 2 * (ny - 2) * nz
    ats_of = lambda i: [(x, inner) for x in pair(i)]
    walls_of = lambda l, ats: take(mask, ats) if l == 1 else None
    y_ats = [(pl.ds(0, nx), 0), (pl.ds(0, nx), ny - 1)]

    travel = [copies(0), copies(1)]
    with jax.named_scope("prologue"):

        for c in range(2):
            half = nx // 2
            xs = range(half * c, half * c + half)
            ats, shapes = [], []
            for x in xs:
                ats += [(x, pl.ds(ny - 1, 1)), (x, pl.ds(0, per_row - 1))]
                shapes += [(1, nz, h), (per_row - 1, nz, h)]
            new, walls = look_up(xs, take(lat, ats))
            store_nodes(ats, shapes, new, walls)
            store_projected(ats, shapes, matmul(new, w_sn[0]))

        with jax.named_scope("bar"):
            pl.semaphore_wait(barrier, len(peers))
        start_z(travel[0])
        start_y(travel[0])

        def two(i):
            if isinstance(i, int):
                return (2 * i - 1, 2 * i) if i > 0 else (0, nx - 1)
            first = jnp.where(i == 0, 0, 2 * i - 1)
            second = jnp.where(i == 0, nx - 1, 2 * i)
            return jnp.where(i < 0, spare[0], first), jnp.where(i < 0, spare[1], second)

        rest = (ny - per_row, nz, h)
        rest_of = lambda xs: [(x, pl.ds(per_row - 1, ny - per_row)) for x in xs]

        @pl.loop(0, nx // 2)
        def _(i):
            xs = two(i)
            ats, before = rest_of(xs), rest_of(two(i - 1))
            done = take(lat, before)
            rows = [g * nx + x for x in xs for g in range(1, per_x)]
            new, walls = look_up(rows, take(lat, ats))
            store_projected(before, [rest] * 2, matmul(done, w_sn[0]))
            store_nodes(ats, [rest] * 2, new, walls)

            @pl.when(i == 1)
            def _():
                start_x(travel[0])

        before = rest_of(two(nx // 2 - 1))
        store_projected(before, [rest] * 2, matmul(take(lat, before), w_sn[0]))
        prepare(0)

    for l in range(2):
        both = travel[l]
        if l == 1:
            with jax.named_scope("start1"):
                start_x(both)
                start_y(both)
                zsend[1, 0] = sz1[0:nx, :, FIRST, :].astype(BF)
                zsend[1, 1] = sz1[0:nx, :, FIRST + nz - 1, :].astype(BF)
                start_z(both)
                prepare(1)
                flags = ones_where(flat[...] >= CODES)
                count = jnp.sum(jnp.sum(flags, axis=0, keepdims=True), axis=1, keepdims=True)
                line[pl.ds(here["gz"], 1), 1:2, :] = jnp.broadcast_to(count, (1, h))[None]
        if l == 1:
            with jax.named_scope("pre1"):

                @pl.loop(1, nx - 1)
                def _(x):
                    edges_xy(l, x)

        with jax.named_scope(f"waitz{l}"):
            wait_z(l, both)
        with jax.named_scope(f"main{l}"):

            @pl.loop(0, nx // 2)
            def _(i):
                @pl.when(i == face)
                def _():
                    with jax.named_scope(f"waitx{l}"):
                        wait_x(both)

                    if l == 1:

                        @pl.loop(0, 2)
                        def _(k):
                            edges_xy(l, k * (nx - 1))

                ats_b, ats_c = ats_of(i - 1), ats_of(i - 2)
                update_c, old_c = upd[0:inner_rows, :], take(lat, ats_c)
                old_b, hidden_b, walls_c = take(lat, ats_b), take(hs, ats_b), walls_of(l, ats_c)
                new_c = latent_of(l, old_c, update_c)
                into = ats_c if l == 0 else ats_of(jnp.where(i < 2, face, i - 2))
                finish(l, into, inner_shape, new_c, walls_c)
                update_b = update_of(l, old_b, hidden_b)
                upd[0:inner_rows, :] = update_b
                for x in pair(i):
                    for y in range(1, ny - 1):
                        begun = hs[x, y] if l == 1 else None
                        hs[x, y] = edges(l, x, y, (4, 5) if l == 1 else range(6), begun)

        with jax.named_scope(f"waity{l}"):
            wait_y(both)
        with jax.named_scope(f"by{l}"):
            ats_b, ats_c = ats_of(face), ats_of(face - 1)
            update_c, old_c = upd[0:inner_rows, :], take(lat, ats_c)
            old_b, hidden_b = take(lat, ats_b), take(hs, ats_b)
            update_b = update_of(l, old_b, hidden_b)
            new_c = latent_of(l, old_c, update_c)
            walls_c, walls_b = walls_of(l, ats_c), walls_of(l, ats_b)
            old_y, walls_y = take(lat, y_ats), walls_of(l, y_ats)
            for y in (0, ny - 1):
                for x in range(nx):
                    hs[x, y] = edges(l, x, y, range(6), None)
            finish(l, ats_c, inner_shape, new_c, walls_c)
            update_y = update_of(l, old_y, take(hs, y_ats))
            finish(l, ats_b, inner_shape, latent_of(l, old_b, update_b), walls_b)
            finish(l, y_ats, (nx, nz, h), latent_of(l, old_y, update_y), walls_y)
        with jax.named_scope(f"waits{l}"):
            wait_sent(both)

    with jax.named_scope("allred"):
        line[pl.ds(here["gz"], 1), 0:1, :] = jnp.sum(wall[...], axis=0, keepdims=True)[None]
        total = exchange(line, here["gz"], sizes["gz"], lambda j: {"gz": j}, 0)
        spot = here["gx"] * sizes["gy"] + here["gy"]
        plane[pl.ds(spot, 1)] = total[None]
        place = lambda j: {"gx": lax.div(j, sizes["gy"]), "gy": lax.rem(j, sizes["gy"])}
        total = exchange(plane, spot, sizes["gx"] * sizes["gy"], place, 1)
        out_wall[...] = total[0:1, :] / total[1:2, :]


def hand_over(latent, mean, out_latent, out_mean, sem):
    step = latent.shape[0] // PARTS
    parts = [pl.ds(k * step, step) for k in range(PARTS)]
    ways = [(mean, out_mean)] + [(latent.at[p], out_latent.at[p]) for p in parts]
    goes = [pltpu.make_async_copy(a, b, sem.at[k]) for k, (a, b) in enumerate(ways)]
    for g in goes:
        g.start()
    for g in goes:
        g.wait()


def solution(mesh):
    sizes = {a: mesh.shape[a] for a in AXES}

    def per_device(*args):
        args = list(args)
        args[8] = jnp.transpose(args[8], (1, 0, 2))
        args = [pltpu.with_memory_space_constraint(a, pltpu.HBM) for a in args]
        nx, ny, nz, h = dims = args[0].shape
        hbm = pl.BlockSpec(memory_space=pltpu.HBM)
        vmem = pl.BlockSpec(memory_space=pltpu.VMEM)
        latent, mean = pl.pallas_call(
            functools.partial(kernel, sizes, dims),
            out_shape=(
                jax.ShapeDtypeStruct(dims, BF),
                jax.ShapeDtypeStruct((1, h), F32),
            ),
            in_specs=[hbm] * 14,
            out_specs=(vmem, vmem),
            scratch_shapes=[pltpu.VMEM(a.shape, a.dtype) for a in args[1:]]
            + [
                pltpu.VMEM((nx + SPARE, ny, PITCH, h), F32),
                pltpu.VMEM((nx + SPARE, ny, PITCH, h), F32),
                pltpu.VMEM((nx * ny * nz // h, h), F32),
                pltpu.VMEM((2 * nx * nz, h), F32),
                pltpu.VMEM((8, h), F32),
                pltpu.VMEM((sizes["gz"], 2, h), F32),
                pltpu.VMEM((sizes["gx"] * sizes["gy"], 2, h), F32),
                pltpu.SemaphoreType.DMA((14,)),
                pltpu.SemaphoreType.DMA((2, 6)),
                pltpu.SemaphoreType.DMA((2, 6)),
                pltpu.SemaphoreType.DMA((2,)),
                pltpu.SemaphoreType.DMA((2,)),
            ],
            compiler_params=pltpu.CompilerParams(
                collective_id=0, has_side_effects=True, vmem_limit_bytes=48 * 1024 * 1024
            ),
            name="mesh_step",
        )(*args)
        latent, mean = pl.pallas_call(
            hand_over,
            out_shape=(
                jax.ShapeDtypeStruct(dims, BF),
                jax.ShapeDtypeStruct((1, h), F32),
            ),
            in_specs=[vmem, vmem],
            out_specs=(hbm, hbm),
            scratch_shapes=[
                pltpu.SemaphoreType.DMA((PARTS + 1,)),
            ],
            compiler_params=pltpu.CompilerParams(vmem_limit_bytes=16 * 1024 * 1024),
            name="hand_over",
        )(latent, mean)
        return latent, mean[0]

    block4 = P(*AXES, None)
    block3 = P(*AXES)
    return jax.shard_map(
        per_device,
        mesh=mesh,
        in_specs=(block4, block3, block3, block3) + (P(),) * 10,
        out_specs=(block4, P()),
        check_vma=False,
    )
```

```python
import functools

import jax
import jax.numpy as jnp
from jax import lax
from jax.experimental import pallas as pl
from jax.experimental.pallas import tpu as pltpu
from jax.sharding import PartitionSpec as P

MESH = pl.DeviceIdType.MESH
AXES = ("gx", "gy", "gz")
EPSILON = 1e-05
BF = jnp.bfloat16
F32 = jnp.float32
PITCH = 48
FIRST = 8
PARTS = 4
SPARE = 5
CODES = 16


def matmul(a, b):
    return jnp.dot(a, b, preferred_element_type=F32)


def silu_of_double(u):
    return u * (jnp.ones_like(u) + jnp.tanh(u))


def kernel(sizes, dims, *refs):
    hbm, (out_lat, out_wall), vmem, rest = refs[:14], refs[14:16], refs[16:29], refs[29:]
    pl.run_scoped(
        functools.partial(body, sizes, dims, hbm, out_lat, out_wall, vmem, rest),
        *scoped(dims),
    )


def scoped(dims):
    nx, ny, nz, h = dims
    more = (nx + SPARE, ny, nz, h)
    wide = (nx + SPARE + 1, ny + 2, nz, h)
    return [
        pltpu.VMEM(s, BF)
        for s in (
            more,
            more,
            more,
            wide,
            wide,
            more,
            more,
            (2, 2, nx, ny, h),
            (2, 2, nx, ny, h),
            (2, h, 2 * h),
            (2, 2 * h, h),
            (2, h, h),
            (2, 6, nz, h),
            (2 * CODES, 2 * h),
        )
    ]


def body(sizes, dims, hbm, out_lat, out_wall, vmem, rest, *bufs):
    (lat, self0, self1, sb0, sb1, hs, mask, zsend, zrecv, w_sn, w_pre, w_out, bias, tables) = bufs
    (sz0, sz1, flat, upd, wall, line, plane, in_sem, send_sem, recv_sem, rsend_sem, rrecv_sem) = rest
    (ntype, bcode, wflag, ttab, btab, eself, enbr, ebias, eout, nself, nagg, nout, ngain) = vmem
    selfs, sbs, szs = (self0, self1), (sb0, sb1), (sz0, sz1)
    nx, ny, nz, h = dims
    here = {a: lax.axis_index(a) for a in AXES}
    gy = here["gy"]
    not_top, not_bottom = gy < sizes["gy"] - 1, gy > 0

    loads = [
        pltpu.make_async_copy(src, dst, in_sem.at[k])
        for k, (src, dst) in enumerate(zip(hbm, (lat.at[pl.ds(0, nx)],) + vmem, strict=True))
    ]
    for k in (1, 2, 3, 0, 4, 5, 6, 7, 8, 9, 10, 11, 12, 13):
        loads[k].start()

    barrier = pltpu.get_barrier_semaphore()
    planes = sizes["gx"] * sizes["gy"]
    peers = [{"gz": lax.rem(here["gz"] + k, sizes["gz"])} for k in range(1, sizes["gz"])]
    for k in range(1, planes):
        j = lax.rem(here["gx"] * sizes["gy"] + here["gy"] + k, planes)
        peers.append({"gx": lax.div(j, sizes["gy"]), "gy": lax.rem(j, sizes["gy"])})
    for peer in peers:
        pl.semaphore_signal(barrier, inc=1, device_id=peer, device_id_type=MESH)

    wall[...] = jnp.zeros_like(wall)

    def exchange(slots, spot, n, place, stage):
        def copy(ref, to):
            return pltpu.make_async_remote_copy(
                src_ref=ref,
                dst_ref=ref,
                send_sem=rsend_sem.at[stage],
                recv_sem=rrecv_sem.at[stage],
                device_id=place(to),
                device_id_type=MESH,
            )

        for k in range(1, n):
            copy(slots.at[spot], lax.rem(spot + k, n)).start()
        copy(slots.at[pl.ds(0, n - 1)], lax.rem(spot + 1, n)).wait()
        total = slots[0]
        for k in range(1, n):
            total = total + slots[k]
        return total

    upd[...] = jnp.zeros_like(upd)
    spare = (nx + 1, nx + 2, nx + 3, nx + 4)
    for x in spare:
        for ref in (lat, hs, mask):
            ref[x] = jnp.zeros((ny, nz, h), BF)

    @pl.when(gy == 0)
    def _():
        @pl.loop(1, nx + 1)
        def _(x):
            sb0[x, 0] = jnp.zeros((nz, h), BF)
            sb1[x, 0] = jnp.zeros((nz, h), BF)

    @pl.when(gy == sizes["gy"] - 1)
    def _():
        @pl.loop(1, nx + 1)
        def _(x):
            sb0[x, ny + 1] = jnp.zeros((nz, h), BF)
            sb1[x, ny + 1] = jnp.zeros((nz, h), BF)

    for k in range(1, 6):
        loads[k].wait()

    columns, per_row = nx * ny, h // nz
    code = (ntype[...] + 4 * bcode[...] + CODES * wflag[...]).astype(F32)
    code = code.reshape(columns, nz).astype(BF)
    iota = lambda shape, d: lax.broadcasted_iota(jnp.int32, shape, d)
    ones_where = lambda hit: jnp.where(hit, 1.0, 0.0)
    repeat = ones_where(lax.rem(iota((nz, h), 1), nz) == iota((nz, h), 0)).astype(BF)
    spread_out = matmul(code, repeat)
    turned = lambda y: lax.rem(y + 1, ny)
    slot = lax.rem(turned(lax.rem(iota((columns, h), 0), ny)), per_row)
    spread_out = jnp.where(slot == lax.div(iota((columns, h), 1), nz), spread_out, 0.0).astype(BF)
    per_x = ny // per_row
    blocks = (nx * per_x, columns)
    row, column = iota(blocks, 0), iota(blocks, 1)
    belongs = jnp.logical_and(
        lax.rem(row, nx) == lax.div(column, ny),
        lax.div(row, nx) == lax.div(turned(lax.rem(column, ny)), per_row),
    )
    flat[...] = matmul(ones_where(belongs).astype(BF), spread_out)

    sums = jnp.concatenate(
        [ttab[...] + btab[b : b + 1, :] for b in range(3)] + [jnp.zeros((4, h), F32)], axis=0
    )
    high = sums.astype(BF)
    low = (sums - high.astype(F32)).astype(BF)
    tables[0:CODES, :h] = high
    tables[CODES : 2 * CODES, :h] = low
    last = iota((2 * CODES, h), 0) == 2 * CODES - 1
    tables[:, h:] = ones_where(last).astype(BF)

    def prepare(l):
        w_pre[l, :h, :] = (nself[l].astype(F32) * 0.5).astype(BF)
        w_pre[l, h:, :] = (matmul(eout[l], nagg[l]) * 0.5).astype(BF)
        w = nout[l].astype(F32)
        w_out[l] = (w - jnp.mean(w, axis=1, keepdims=True)).astype(BF)
        for d in range(6):
            row = ebias[d, l : l + 1, :] * 0.5
            bias[l, d] = jnp.broadcast_to(row, (nz, h)).astype(BF)

    for k in range(6, 14):
        loads[k].wait()
    for l in range(2):
        w_sn[l, :, :h] = (eself[l].astype(F32) * 0.5).astype(BF)
        w_sn[l, :, h:] = (enbr[l].astype(F32) * 0.5).astype(BF)
    loads[0].wait()

    for k, z in enumerate((0, nz - 1)):
        kind = jnp.broadcast_to(code[:, z : z + 1].astype(F32), (columns, 2 * CODES))
        kind = jnp.where(kind >= CODES, kind - CODES, kind)
        hot = ones_where(kind == lax.rem(iota((columns, 2 * CODES), 1), CODES).astype(F32))
        found = matmul(hot.astype(BF), tables[:, :h])
        face = lat[0:nx, :, z, :].astype(F32).reshape(columns, h)
        new = (face + found).astype(BF)
        zsend[0, k] = matmul(new, w_sn[0, :, h:]).astype(BF).reshape(nx, ny, h)

    def take(ref, ats):
        return jnp.concatenate([ref[at].reshape(-1, h) for at in ats], axis=0)

    def look_up(rows, old):
        nodes = len(rows) * h
        nodes_code = jnp.concatenate([flat[pl.ds(r, 1), :] for r in rows], axis=1)
        nodes_code = jnp.broadcast_to(nodes_code, (2 * CODES, nodes))
        on_wall = nodes_code >= CODES
        kind = jnp.where(on_wall, nodes_code - CODES, nodes_code)
        at = iota((2 * CODES, nodes), 0)
        hit = kind == lax.rem(at, CODES).astype(F32)
        hot = jnp.where(at == 2 * CODES - 1, ones_where(on_wall), ones_where(hit)).astype(BF)
        found = lax.dot_general(
            hot, tables[...], (((0,), (0,)), ((), ())), preferred_element_type=F32
        )
        return (old.astype(F32) + found[:, :h]).astype(BF), found[:, h:].astype(BF)

    def pieces(ats, shapes):
        first = 0
        for at, shape in zip(ats, shapes, strict=True):
            yield at, shape, slice(first, first + shape[0] * nz)
            first += shape[0] * nz

    def store_nodes(ats, shapes, new, walls):
        for at, shape, part in pieces(ats, shapes):
            lat[at] = new[part].reshape(shape)
            mask[at] = walls[part].reshape(shape)

    def store_projected(ats, shapes, both):
        for at, shape, part in pieces(ats, shapes):
            store_parts(0, at, shape, both[part])

    def store_parts(r, at, shape, both):
        x, y = at
        s = both[:, h:].reshape(shape)
        selfs[r][x, y] = both[:, :h].astype(BF).reshape(shape)
        sbs[r][shift(x), shift(y)] = s.astype(BF)
        szs[r][x, y, FIRST : FIRST + nz, :] = s

    def shift(i):
        return pl.ds(i.start + 1, i.size) if isinstance(i, pl.Slice) else i + 1

    def copies(r):
        up = {a: lax.rem(here[a] + 1, sizes[a]) for a in AXES}
        down = {a: lax.rem(here[a] + sizes[a] - 1, sizes[a]) for a in AXES}
        sb = sbs[r]
        rows_x, rows_y = pl.ds(1, nx), pl.ds(1, ny)
        plans = (
            ("gx", up, sb.at[nx, rows_y], sb.at[0, rows_y]),
            ("gx", down, sb.at[1, rows_y], sb.at[nx + 1, rows_y]),
            ("gy", up, sb.at[rows_x, ny], sb.at[rows_x, 0]),
            ("gy", down, sb.at[rows_x, 1], sb.at[rows_x, ny + 1]),
            ("gz", up, zsend.at[r, 1], zrecv.at[r, 0]),
            ("gz", down, zsend.at[r, 0], zrecv.at[r, 1]),
        )
        return [
            pltpu.make_async_remote_copy(
                src_ref=src,
                dst_ref=dst,
                send_sem=send_sem.at[r, k],
                recv_sem=recv_sem.at[r, k],
                device_id={a: to[a]},
                device_id_type=MESH,
            )
            for k, (a, to, src, dst) in enumerate(plans)
        ]

    def start_z(both):
        both[4].start()
        both[5].start()

    def start_x(both):
        both[0].start()
        both[1].start()

    def start_y(both):
        @pl.when(not_top)
        def _():
            both[2].start()

        @pl.when(not_bottom)
        def _():
            both[3].start()

    def wait_z(r, both):
        both[4].wait_recv()
        both[5].wait_recv()
        szs[r][0:nx, :, FIRST - 1, :] = zrecv[r, 0].astype(F32)
        szs[r][0:nx, :, FIRST + nz, :] = zrecv[r, 1].astype(F32)

    def wait_x(both):
        both[0].wait_recv()
        both[1].wait_recv()

    def wait_y(both):
        @pl.when(not_bottom)
        def _():
            both[2].wait_recv()

        @pl.when(not_top)
        def _():
            both[3].wait_recv()

    def wait_sent(both):
        for k in (0, 1, 4, 5):
            both[k].wait_send()

        @pl.when(not_top)
        def _():
            both[2].wait_send()

        @pl.when(not_bottom)
        def _():
            both[3].wait_send()

    def edges(l, x, y, dirs, total):
        base = selfs[l][x, y]
        for d in dirs:
            if d < 4:
                near = sbs[l][x + (0, 2, 1, 1)[d], y + (1, 1, 0, 2)[d]]
            else:
                first = FIRST + (-1, 1)[d - 4]
                near = szs[l][x, y, first : first + nz, :].astype(BF)
            term = silu_of_double((base + bias[l, d]) + near)
            if d == 2 and y == 0:
                term = term * keep(not_bottom)
            if d == 3 and y == ny - 1:
                term = term * keep(not_top)
            total = term if total is None else total + term
        return total

    def edges_xy(l, x):
        for y in range(1, ny - 1):
            hs[x, y] = edges(l, x, y, (0, 1, 2, 3), None)

    def keep(cond):
        return jnp.full((nz, h), cond.astype(F32)).astype(BF)

    def update_of(l, old, hidden):
        p = matmul(jnp.concatenate([old, hidden], axis=1), w_pre[l]).astype(BF)
        return matmul(silu_of_double(p), w_out[l])

    def latent_of(l, old, update):
        spread = jnp.mean(update * update, axis=1, keepdims=True)
        normed = update * lax.rsqrt(spread + EPSILON) * ngain[l : l + 1, :]
        return (old.astype(F32) + normed).astype(BF)

    def finish(l, ats, shape, new, walls):
        rows = new.shape[0] // len(ats)
        both = matmul(new, w_sn[1]) if l == 0 else None
        if l == 1:
            wall[...] += jnp.sum((new * walls).astype(F32).reshape(-1, 8, h), axis=0)
        for k, at in enumerate(ats):
            part = slice(k * rows, (k + 1) * rows)
            if l == 0:
                lat[at] = new[part].reshape(shape)
                store_parts(1, at, shape, both[part])
            else:
                out_lat[at] = new[part].reshape(shape)

    face = nx // 2 - 1

    def pair(i):
        if isinstance(i, int):
            return (0, nx - 1) if i == face else (2 * i + 1, 2 * i + 2)
        first = jnp.where(i == face, 0, 2 * i + 1)
        second = jnp.where(i == face, nx - 1, 2 * i + 2)
        return jnp.where(i < 0, spare[0], first), jnp.where(i < 0, spare[1], second)

    inner = pl.ds(1, ny - 2)
    inner_shape = (ny - 2, nz, h)
    inner_rows = 2 * (ny - 2) * nz
    ats_of = lambda i: [(x, inner) for x in pair(i)]
    walls_of = lambda l, ats: take(mask, ats) if l == 1 else None
    y_ats = [(pl.ds(0, nx), 0), (pl.ds(0, nx), ny - 1)]

    travel = [copies(0), copies(1)]
    with jax.named_scope("prologue"):

        for c in range(2):
            half = nx // 2
            xs = range(half * c, half * c + half)
            ats, shapes = [], []
            for x in xs:
                ats += [(x, pl.ds(ny - 1, 1)), (x, pl.ds(0, per_row - 1))]
                shapes += [(1, nz, h), (per_row - 1, nz, h)]
            new, walls = look_up(xs, take(lat, ats))
            store_nodes(ats, shapes, new, walls)
            store_projected(ats, shapes, matmul(new, w_sn[0]))

        with jax.named_scope("bar"):
            pl.semaphore_wait(barrier, len(peers))
        start_z(travel[0])
        start_y(travel[0])

        def four(i):
            first = (0, nx - 1, 1, 2)
            if isinstance(i, int):
                return first if i == 0 else tuple(4 * i - 1 + k for k in range(4))
            later = [jnp.where(i == 0, first[k], 4 * i - 1 + k) for k in range(4)]
            return tuple(jnp.where(i < 0, spare[k], x) for k, x in enumerate(later))

        rest = (ny - per_row, nz, h)
        rest_of = lambda xs: [(x, pl.ds(per_row - 1, ny - per_row)) for x in xs]

        @pl.loop(0, nx // 4)
        def _(i):
            xs = four(i)
            ats, before = rest_of(xs), rest_of(four(i - 1))
            done = take(lat, before)
            rows = [g * nx + x for x in xs for g in range(1, per_x)]
            new, walls = look_up(rows, take(lat, ats))
            store_projected(before, [rest] * 4, matmul(done, w_sn[0]))
            store_nodes(ats, [rest] * 4, new, walls)

            @pl.when(i == 1)
            def _():
                start_x(travel[0])

        before = rest_of(four(nx // 4 - 1))
        store_projected(before, [rest] * 4, matmul(take(lat, before), w_sn[0]))
        prepare(0)

    for l in range(2):
        both = travel[l]
        if l == 1:
            with jax.named_scope("start1"):
                zsend[1, 0] = sz1[0:nx, :, FIRST, :].astype(BF)
                zsend[1, 1] = sz1[0:nx, :, FIRST + nz - 1, :].astype(BF)
                start_z(both)
                prepare(1)
                flags = ones_where(flat[...] >= CODES)
                count = jnp.sum(jnp.sum(flags, axis=0, keepdims=True), axis=1, keepdims=True)
                line[pl.ds(here["gz"], 1), 1:2, :] = jnp.broadcast_to(count, (1, h))[None]
        if l == 1:
            with jax.named_scope("pre1"):

                @pl.loop(1, nx - 1)
                def _(x):
                    edges_xy(l, x)

        with jax.named_scope(f"waitz{l}"):
            wait_z(l, both)
        with jax.named_scope(f"main{l}"):

            @pl.loop(0, nx // 2)
            def _(i):
                @pl.when(i == face)
                def _():
                    with jax.named_scope(f"waitx{l}"):
                        wait_x(both)

                    if l == 1:

                        @pl.loop(0, 2)
                        def _(k):
                            edges_xy(l, k * (nx - 1))

                ats_b, ats_c = ats_of(i - 1), ats_of(i - 2)
                update_c, old_c = upd[0:inner_rows, :], take(lat, ats_c)
                old_b, hidden_b, walls_c = take(lat, ats_b), take(hs, ats_b), walls_of(l, ats_c)
                new_c = latent_of(l, old_c, update_c)
                into = ats_c if l == 0 else ats_of(jnp.where(i < 2, face, i - 2))
                finish(l, into, inner_shape, new_c, walls_c)
                update_b = update_of(l, old_b, hidden_b)
                upd[0:inner_rows, :] = update_b
                for x in pair(i):
                    for y in range(1, ny - 1):
                        begun = hs[x, y] if l == 1 else None
                        hs[x, y] = edges(l, x, y, (4, 5) if l == 1 else range(6), begun)

        with jax.named_scope(f"waity{l}"):
            wait_y(both)
        with jax.named_scope(f"by{l}"):
            ats_b, ats_c = ats_of(face), ats_of(face - 1)
            update_c, old_c = upd[0:inner_rows, :], take(lat, ats_c)
            old_b, hidden_b = take(lat, ats_b), take(hs, ats_b)
            update_b = update_of(l, old_b, hidden_b)
            new_c = latent_of(l, old_c, update_c)
            walls_c, walls_b = walls_of(l, ats_c), walls_of(l, ats_b)
            old_y, walls_y = take(lat, y_ats), walls_of(l, y_ats)
            for y in (0, ny - 1):
                for x in range(nx):
                    hs[x, y] = edges(l, x, y, range(6), None)
            update_y = update_of(l, old_y, take(hs, y_ats))
            finish(l, ats_b, inner_shape, latent_of(l, old_b, update_b), walls_b)
            finish(l, y_ats, (nx, nz, h), latent_of(l, old_y, update_y), walls_y)
            if l == 0:
                start_x(travel[1])
                start_y(travel[1])
            finish(l, ats_c, inner_shape, new_c, walls_c)
        with jax.named_scope(f"waits{l}"):
            wait_sent(both)

    with jax.named_scope("allred"):
        line[pl.ds(here["gz"], 1), 0:1, :] = jnp.sum(wall[...], axis=0, keepdims=True)[None]
        total = exchange(line, here["gz"], sizes["gz"], lambda j: {"gz": j}, 0)
        spot = here["gx"] * sizes["gy"] + here["gy"]
        plane[pl.ds(spot, 1)] = total[None]
        place = lambda j: {"gx": lax.div(j, sizes["gy"]), "gy": lax.rem(j, sizes["gy"])}
        total = exchange(plane, spot, sizes["gx"] * sizes["gy"], place, 1)
        out_wall[...] = total[0:1, :] / total[1:2, :]


def hand_over(latent, mean, out_latent, out_mean, sem):
    step = latent.shape[0] // PARTS
    parts = [pl.ds(k * step, step) for k in range(PARTS)]
    ways = [(mean, out_mean)] + [(latent.at[p], out_latent.at[p]) for p in parts]
    goes = [pltpu.make_async_copy(a, b, sem.at[k]) for k, (a, b) in enumerate(ways)]
    for g in goes:
        g.start()
    for g in goes:
        g.wait()


def solution(mesh):
    sizes = {a: mesh.shape[a] for a in AXES}

    def per_device(*args):
        args = list(args)
        args[8] = jnp.transpose(args[8], (1, 0, 2))
        args = [pltpu.with_memory_space_constraint(a, pltpu.HBM) for a in args]
        nx, ny, nz, h = dims = args[0].shape
        hbm = pl.BlockSpec(memory_space=pltpu.HBM)
        vmem = pl.BlockSpec(memory_space=pltpu.VMEM)
        latent, mean = pl.pallas_call(
            functools.partial(kernel, sizes, dims),
            out_shape=(
                jax.ShapeDtypeStruct(dims, BF),
                jax.ShapeDtypeStruct((1, h), F32),
            ),
            in_specs=[hbm] * 14,
            out_specs=(vmem, vmem),
            scratch_shapes=[pltpu.VMEM(a.shape, a.dtype) for a in args[1:]]
            + [
                pltpu.VMEM((nx + SPARE, ny, PITCH, h), F32),
                pltpu.VMEM((nx + SPARE, ny, PITCH, h), F32),
                pltpu.VMEM((nx * ny * nz // h, h), F32),
                pltpu.VMEM((2 * nx * nz, h), F32),
                pltpu.VMEM((8, h), F32),
                pltpu.VMEM((sizes["gz"], 2, h), F32),
                pltpu.VMEM((sizes["gx"] * sizes["gy"], 2, h), F32),
                pltpu.SemaphoreType.DMA((14,)),
                pltpu.SemaphoreType.DMA((2, 6)),
                pltpu.SemaphoreType.DMA((2, 6)),
                pltpu.SemaphoreType.DMA((2,)),
                pltpu.SemaphoreType.DMA((2,)),
            ],
            compiler_params=pltpu.CompilerParams(
                collective_id=0, has_side_effects=True, vmem_limit_bytes=48 * 1024 * 1024
            ),
            name="mesh_step",
        )(*args)
        latent, mean = pl.pallas_call(
            hand_over,
            out_shape=(
                jax.ShapeDtypeStruct(dims, BF),
                jax.ShapeDtypeStruct((1, h), F32),
            ),
            in_specs=[vmem, vmem],
            out_specs=(hbm, hbm),
            scratch_shapes=[
                pltpu.SemaphoreType.DMA((PARTS + 1,)),
            ],
            compiler_params=pltpu.CompilerParams(vmem_limit_bytes=16 * 1024 * 1024),
            name="hand_over",
        )(latent, mean)
        return latent, mean[0]

    block4 = P(*AXES, None)
    block3 = P(*AXES)
    return jax.shard_map(
        per_device,
        mesh=mesh,
        in_specs=(block4, block3, block3, block3) + (P(),) * 10,
        out_specs=(block4, P()),
        check_vma=False,
    )
```
